32 devices in a mesh: grp: 2 (over y), seq: 8 (over z, x), head: 2 (over core).
Axes of the slice: x: 2, y: 2, z: 4, core: 2. Of those that a mesh axis runs over, the one named last changes fastest.
Arguments:
- key_cache: bfloat16 [4, 64, 128, 1024], P('grp', ('seq', 'head')), parts along dimension 0, may hold values from -160 to 160, as said below
- value_cache: bfloat16 [4, 64, 128, 1024], P('grp', ('seq', 'head')), parts along dimension 0, may hold values from -16 to 16, as said below
- query: bfloat16 [4, 4096], P('grp', 'head'), parts along dimension 0, may hold values from -48 to 48, as said below
- lengths: int32 [4], P('grp'), parts along dimension 0, may hold values from 128 to 8192, as said below
- block_map: int32 [4, 64], P('grp'), parts along dimension 0, may hold values from 0 to 63, each once within a row
Outputs:
- attended: bfloat16 [4, 4096], P('grp', 'head'), parts along dimension 0
The draws below stay inside these ranges and needn't reach their ends.
There are 2 independent parts, one for each index of `grp`. The reference program is written for one: setup_inputs(seed, part) draws one part's arguments, and reference() takes and returns one part's arrays. A program takes and returns all parts, laid end to end along the dimension named above; each array names one. Nothing has to cross between parts.
Inputs may be any that keep to these rules, and one draw needn't show every extreme that they name: `lengths`: every length is a multiple of 128; in every draw some request has length 8192. `key_cache`: finite entries, drawn afresh for every request, block, token and channel. `value_cache`: finite entries, drawn afresh for every request, block, token and channel. `query`: finite entries, drawn afresh for every request, head and channel.
All inputs are finite; a program needn't handle non-finite values.
Results may differ from the reference program's by a relative error of at most 0.0055.
Values may be sent and summed in bfloat16 or wider, within the bound.
A program may use at most 64 MiB of HBM per device.

```python
import jax
import jax.numpy as jnp
from jax import lax

QH = 32
KVH = 8
HD = 128
BLK = 128
BATCH = 2
NBLK = 64


def layout_terms(key):
    first_key, second_key, third_key = jax.random.split(jax.random.fold_in(key, 11), 3)
    direction = jax.random.normal(first_key, (KVH, HD), jnp.float32)
    direction = direction / jnp.sqrt(jnp.sum(direction * direction, axis=1, keepdims=True))
    coeffs = jax.random.uniform(second_key, (BATCH, NBLK, KVH), jnp.float32, -1.5, 1.5)
    return (direction, coeffs)


def draw_key_cache(key, part):
    direction, coeffs = layout_terms(key)
    shape = (BATCH, NBLK, BLK, KVH, HD)
    noise = jax.random.normal(jax.random.fold_in(key, 21), shape, jnp.float32)
    keys_full = noise + coeffs[:, :, None, :, None] * direction[None, None, None, :, :]
    return keys_full.reshape(BATCH, NBLK, BLK, KVH * HD).astype(jnp.bfloat16)


def draw_value_cache(key, part):
    means = jax.random.normal(jax.random.fold_in(key, 31), (BATCH, NBLK, KVH * HD), jnp.float32)
    noise = 0.5 * jax.random.normal(jax.random.fold_in(key, 32), (BATCH, NBLK, BLK, KVH * HD), jnp.float32)
    return (noise + means[:, :, None, :]).astype(jnp.bfloat16)


def draw_query(key, part):
    direction, coeffs = layout_terms(key)
    noise = jax.random.normal(jax.random.fold_in(key, 41), (BATCH, KVH, QH // KVH, HD), jnp.float32)
    full = noise + 2.0 * HD ** 0.5 * direction[None, :, None, :]
    return full.reshape(BATCH, QH * HD).astype(jnp.bfloat16)


def draw_lengths(key, part):
    first_key, second_key = jax.random.split(jax.random.fold_in(key, 51))
    counts = jax.random.randint(first_key, (BATCH,), 1, NBLK + 1)
    fullest = jax.random.randint(second_key, (), 0, BATCH)
    counts = jnp.where(jnp.arange(BATCH) == fullest, NBLK, counts)
    return (counts * BLK).astype(jnp.int32)


def setup_inputs(seed: int = 0, part: int = 0) -> dict:
    splits = jax.random.split(jax.random.key(seed), 6)
    part_splits = jax.random.split(jax.random.fold_in(splits[5], part), 6)
    key_cache = draw_key_cache(jax.random.fold_in(jax.random.fold_in(splits[5], part), 71), part)
    value_cache = draw_value_cache(jax.random.fold_in(jax.random.fold_in(splits[5], part), 71), part)
    query = draw_query(jax.random.fold_in(jax.random.fold_in(splits[5], part), 71), part)
    lengths = draw_lengths(jax.random.fold_in(jax.random.fold_in(splits[5], part), 71), part)
    block_map = jax.vmap(lambda own: jax.random.permutation(own, NBLK))(jax.random.split(part_splits[4], BATCH)).reshape((BATCH, NBLK)).astype(jnp.int32)
    return dict(key_cache=key_cache, value_cache=value_cache, query=query, lengths=lengths, block_map=block_map)


def reference(key_cache, value_cache, query, lengths, block_map):
    key_rows = key_cache.reshape(BATCH, NBLK * BLK, KVH, HD)
    value_rows = value_cache.reshape(BATCH, NBLK * BLK, KVH, HD)
    live_blocks = block_map < (lengths // BLK)[:, None]
    live_tokens = jnp.repeat(live_blocks, BLK, axis=1)[:, None, :]
    queries = query.reshape(BATCH, KVH, QH // KVH, HD).astype(jnp.float32)
    score_scale = 1.0 / (HD ** 0.5)

    def one_group(group):
        key_portion = key_rows[:, :, group, :].astype(jnp.float32)
        value_portion = value_rows[:, :, group, :].astype(jnp.float32)
        query_portion = queries[:, group]
        logit_scores = jnp.einsum("rcy,rly->rcl", query_portion, key_portion, precision=lax.Precision.HIGHEST) * score_scale
        row_top = jnp.max(jnp.where(live_tokens, logit_scores, jnp.float32(-1e30)), axis=-1)
        expo = jnp.where(live_tokens, jnp.exp(logit_scores - row_top[..., None]), jnp.float32(0.0))
        total = jnp.sum(expo, axis=-1)
        rounded_scores = lax.optimization_barrier(expo.astype(jnp.bfloat16)).astype(jnp.float32)
        summed_values = jnp.einsum("wog,wgn->won", rounded_scores, value_portion, precision=lax.Precision.HIGHEST)
        return summed_values / total[..., None]

    outputs = lax.map(one_group, jnp.arange(KVH, dtype=jnp.int32))
    outputs = jnp.transpose(outputs, (1, 0, 2, 3)).reshape(BATCH, QH * HD)
    return outputs.astype(jnp.bfloat16)
```

```python
import functools

import jax
import jax.numpy as jnp
from jax import lax
from jax.experimental import pallas as pl
from jax.experimental.pallas import tpu as pltpu
from jax.sharding import PartitionSpec as P

QH = 32
KVH = 8
HD = 128
BLK = 128
REP = QH // KVH
MESH = pl.DeviceIdType.MESH
NEG = -1e30
LOG2E = 1.4426950408889634


def kernel(
    n_seq, n_head,
    lengths_hbm, map_hbm, q_hbm, k_hbm, v_hbm, out_ref,
    lengths, block_map, q_ref, small_sem,
    k_buf, v_buf, q_mate, num_send, stat_send, num_recv, stat_recv, share_ref, order_ref,
    kv_sem, q_sem, nsend_sem, nrecv_sem, ssend_sem, srecv_sem, ready_sem,
):
    seq = lax.axis_index("seq")
    head = lax.axis_index("head")
    batch, slots = k_hbm.shape[0], k_hbm.shape[1]
    width = k_hbm.shape[3] // n_head
    groups = width // HD
    rows_b = groups * REP
    rows = batch * rows_b
    tokens = slots * BLK
    me = seq * n_head + head
    mate = n_head - 1 - head
    n_all = n_seq * n_head
    small = n_all <= 16

    def loop(lo, hi, body):
        if small:
            for i in range(lo, hi):
                body(i)
        else:
            def step(i, carry):
                body(i)
                return carry
            lax.fori_loop(lo, hi, step, 0)

    def turned(d):
        there = seq + d
        return jnp.where(there >= n_seq, there - n_seq, there)

    smalls = [pltpu.make_async_copy(a, b, small_sem.at[i]) for i, (a, b) in enumerate(
        ((lengths_hbm, lengths), (map_hbm, block_map), (q_hbm, q_ref)))]

    def load(half, which):
        owner = jnp.where(half == 0, head, mate)
        source, target = ((k_hbm, k_buf), (v_hbm, v_buf))[which]
        lanes = pl.ds(pl.multiple_of(owner * width, width), width)
        return pltpu.make_async_copy(
            source.at[:, :, :, lanes], target.at[half], kv_sem.at[half, which]
        )

    for copy in smalls:
        copy.start()
    load(0, 0).start()
    for half, which in ((1, 0), (0, 1)):
        load(half, which).start(priority=1)

    barrier = pltpu.get_barrier_semaphore()
    lead = head == n_head - 1

    def q_copy():
        return pltpu.make_async_remote_copy(
            src_ref=q_ref, dst_ref=q_mate, send_sem=q_sem.at[0], recv_sem=q_sem.at[1],
            device_id={"head": mate}, device_id_type=MESH,
        )

    def tell_mate():
        pl.semaphore_signal(ready_sem, inc=1, device_id={"head": mate}, device_id_type=MESH)

    @pl.when(lead)
    def _():
        pl.semaphore_signal(barrier, inc=1, device_id={"head": mate}, device_id_type=MESH)
        pl.semaphore_wait(ready_sem, 1)

        def greet(d):
            pl.semaphore_signal(barrier, inc=1, device_id={"seq": turned(d)}, device_id_type=MESH)

        loop(1, n_seq, greet)

    @pl.when(jnp.logical_not(lead))
    def _():
        pl.semaphore_wait(barrier, 1)
        tell_mate()

    smalls[2].wait()
    q_copy().start()

    def everyone_in():
        @pl.when(lead)
        def _():
            pl.semaphore_wait(barrier, n_seq - 1)
            tell_mate()

        @pl.when(jnp.logical_not(lead))
        def _():
            pl.semaphore_wait(ready_sem, 1)

    def bias_of(b):
        parts = []
        for j in range(slots):
            here = block_map[b, me * slots + j] * BLK < lengths[b]
            parts.append(jnp.broadcast_to(jnp.where(here, 0.0, NEG), (rows_b, BLK)))
        return jnp.concatenate(parts, axis=1)

    def diagonal(q):
        lifted = q.astype(jnp.float32).reshape(rows, HD)
        wide = jnp.concatenate([lifted] * groups, axis=1)
        row_group = lax.rem(lax.broadcasted_iota(jnp.int32, wide.shape, 0), rows_b) // REP
        lane_group = lax.broadcasted_iota(jnp.int32, wide.shape, 1) // HD
        return jnp.where(row_group == lane_group, wide, 0.0).astype(jnp.bfloat16)

    for copy in smalls[:2]:
        copy.wait()
    load(1, 1).start(priority=1)
    bias = [bias_of(b) for b in range(batch)]

    def copies(half, d):
        where = {"seq": turned(d), "head": mate if half else head}
        return (
            pltpu.make_async_remote_copy(
                src_ref=stat_send.at[pl.ds(half, 1)], dst_ref=stat_recv.at[pl.ds(me, 1)],
                send_sem=ssend_sem, recv_sem=srecv_sem, device_id=where, device_id_type=MESH,
            ),
            pltpu.make_async_remote_copy(
                src_ref=num_send.at[half], dst_ref=num_recv.at[me],
                send_sem=nsend_sem, recv_sem=nrecv_sem, device_id=where, device_id_type=MESH,
            ),
        )

    def send(half, which):
        loop(1, n_seq, lambda d: copies(half, d)[which].start())
        if half:
            copies(half, 0)[which].start()

    def score(half, spread):
        load(half, 0).wait()
        return [lax.dot_general(
            spread[b * rows_b:(b + 1) * rows_b], k_buf[half, b].reshape(tokens, width),
            (((1,), (1,)), ((), ())), preferred_element_type=jnp.float32,
        ) for b in range(batch)]

    def soften(half, raw):
        expos, tops, totals = [], [], []
        for b in range(batch):
            scores = raw[b] * (LOG2E / HD**0.5) + bias[b]
            top = jnp.max(scores, axis=1, keepdims=True)
            expo = jnp.exp2(scores - top)
            tops.append(top)
            totals.append(jnp.sum(expo, axis=1, keepdims=True))
            expos.append(expo.astype(jnp.bfloat16))
        column = jnp.concatenate(tops + totals + [jnp.zeros((HD - 2 * rows, 1), jnp.float32)], axis=0)
        stat_send[half:half + 1] = jnp.transpose(jnp.broadcast_to(column, (HD, HD)))[0:1]
        return expos

    def weigh(half, expos):
        load(half, 1).wait()
        row_group = lax.broadcasted_iota(jnp.int32, (rows_b, HD), 0) // REP
        nums = []
        for b in range(batch):
            values = v_buf[half, b].reshape(tokens, width)
            full = jnp.dot(expos[b], values, preferred_element_type=jnp.float32)
            part = jnp.zeros((rows_b, HD), jnp.float32)
            for g in range(groups):
                part = jnp.where(row_group == g, full[:, g * HD:(g + 1) * HD], part)
            nums.append(part)
        num_send[half] = jnp.concatenate(nums, axis=0).astype(jnp.bfloat16)
        send(half, 1)

    raw_own = score(0, diagonal(q_ref[...]))
    q_copy().wait()
    raw_mate = score(1, diagonal(q_mate[...]))
    expos = soften(0, raw_own)
    everyone_in()
    send(0, 0)
    weigh(0, expos)
    expos = soften(1, raw_mate)
    send(1, 0)
    weigh(1, expos)

    all_nums = pltpu.make_async_remote_copy(
        src_ref=num_recv.at[pl.ds(0, n_all - 1)], dst_ref=num_recv.at[pl.ds(0, n_all - 1)],
        send_sem=nsend_sem, recv_sem=nrecv_sem, device_id={"head": mate}, device_id_type=MESH,
    )
    all_stats = pltpu.make_async_remote_copy(
        src_ref=stat_recv.at[pl.ds(0, n_all - 1)], dst_ref=stat_recv.at[pl.ds(0, n_all - 1)],
        send_sem=ssend_sem, recv_sem=srecv_sem, device_id={"head": mate}, device_id_type=MESH,
    )
    all_stats.wait_send()
    all_nums.wait_send()
    stat_recv[pl.ds(me, 1)] = stat_send[0:1]
    num_recv[me] = num_send[0]
    all_stats.wait_recv()
    stats = stat_recv[...]
    top = stats[:, :rows]
    total = stats[:, rows:2 * rows]
    factor = jnp.exp2(top - jnp.max(top, axis=0, keepdims=True))
    share = factor / jnp.sum(factor * total, axis=0, keepdims=True)
    share_columns = jnp.transpose(jnp.concatenate(
        [share, jnp.zeros((n_all, HD - rows), jnp.float32)], axis=1))[:rows]
    for s in range(n_all):
        share_ref[s] = jnp.broadcast_to(share_columns[:, s:s + 1], (rows, HD))
    all_nums.wait_recv()

    def term(s):
        return share_ref[s] * num_recv[s].astype(jnp.float32)

    if small:
        terms = [term(s) for s in range(n_all)]
        while len(terms) > 1:
            terms = [a + b for a, b in zip(terms[::2], terms[1::2])] + terms[len(terms) // 2 * 2:]
        result = terms[0]
    else:
        result = lax.fori_loop(0, n_all, lambda s, acc: acc + term(s), jnp.zeros((rows, HD), jnp.float32))
    for b in range(batch):
        order_ref[pl.ds(b, rows_b, stride=batch), :] = result[b * rows_b:(b + 1) * rows_b]
    out_ref[...] = order_ref[...].astype(out_ref.dtype)


def solution(mesh):
    n_seq, n_head = mesh.shape["seq"], mesh.shape["head"]
    n_all = n_seq * n_head

    def on_device(key_cache, value_cache, query, lengths, block_map):
        batch, slots, _, channels = key_cache.shape
        width = channels // n_head
        rows_b = (width // HD) * REP
        rows = batch * rows_b
        dma = pltpu.SemaphoreType.DMA
        result = pl.pallas_call(
            functools.partial(kernel, n_seq, n_head),
            out_shape=pltpu.VMEM((rows, HD), jnp.bfloat16),
            in_specs=[
                *[pl.BlockSpec(memory_space=pl.ANY)] * 5,
            ],
            out_specs=pl.BlockSpec(memory_space=pltpu.VMEM),
            scratch_shapes=[
                pltpu.SMEM(lengths.shape, jnp.int32),
                pltpu.SMEM(block_map.shape, jnp.int32),
                pltpu.VMEM(query.shape, jnp.bfloat16),
                dma((3,)),
                pltpu.VMEM((n_head, batch, slots, BLK, width), jnp.bfloat16),
                pltpu.VMEM((n_head, batch, slots, BLK, width), jnp.bfloat16),
                pltpu.VMEM(query.shape, jnp.bfloat16),
                pltpu.VMEM((n_head, rows, HD), jnp.bfloat16),
                pltpu.VMEM((n_head, HD), jnp.float32),
                pltpu.VMEM((n_all, rows, HD), jnp.bfloat16),
                pltpu.VMEM((n_all, HD), jnp.float32),
                pltpu.VMEM((n_all, rows, HD), jnp.float32),
                pltpu.VMEM((rows, HD), jnp.float32),
                dma((n_head, 2)),
                dma((2,)),
                dma(()),
                dma(()),
                dma(()),
                dma(()),
                pltpu.SemaphoreType.REGULAR,
            ],
            compiler_params=pltpu.CompilerParams(collective_id=0, has_side_effects=True),
        )(lengths, block_map, query, key_cache, value_cache)
        return result.reshape(rows_b, batch, HD).transpose(1, 0, 2).reshape(batch, rows_b * HD)

    placed = (
        P("grp", ("seq", "head"), None, None),
        P("grp", ("seq", "head"), None, None),
        P("grp", "head"),
        P("grp"),
        P("grp", None),
    )
    return jax.shard_map(
        on_device, mesh=mesh, in_specs=placed, out_specs=P("grp", "head"), check_vma=False
    )
```

```python
import functools

import jax
import jax.numpy as jnp
from jax import lax
from jax.experimental import pallas as pl
from jax.experimental.pallas import tpu as pltpu
from jax.sharding import PartitionSpec as P

QH = 32
KVH = 8
HD = 128
BLK = 128
TILE = 256
REP = QH // KVH
MESH = pl.DeviceIdType.MESH
NEG = -1e30
LOG2E = 1.4426950408889634


def kernel(
    n_seq, n_head, score_acc, value_acc,
    lengths_hbm, map_hbm, q_hbm, k_hbm, v_hbm, out_ref,
    lengths, block_map, q_ref, small_sem,
    k_buf, v_buf, q_mate, num_send, stat_send, num_recv, stat_recv, share_ref, order_ref,
    kv_sem, q_sem, nsend_sem, nrecv_sem, ssend_sem, srecv_sem, ready_sem,
):
    seq = lax.axis_index("seq")
    head = lax.axis_index("head")
    batch, slots = k_hbm.shape[0], k_hbm.shape[1]
    width = k_hbm.shape[3] // n_head
    groups = width // HD
    rows_b = groups * REP
    rows = batch * rows_b
    tokens = slots * BLK
    per = TILE // BLK
    pieces = tokens // TILE
    strips = width // TILE
    me = seq * n_head + head
    mate = n_head - 1 - head
    n_all = n_seq * n_head
    small = n_all <= 16

    def loop(lo, hi, body):
        if small:
            for i in range(lo, hi):
                body(i)
        else:
            def step(i, carry):
                body(i)
                return carry
            lax.fori_loop(lo, hi, step, 0)

    def turned(d):
        if small and n_seq & (n_seq - 1) == 0:
            there = seq
            for bit in range(n_seq.bit_length() - 1):
                if d >> bit & 1:
                    there = there + (1 << bit) * (1 - 2 * (seq // (1 << bit) % 2))
            return there
        there = seq + d
        return jnp.where(there >= n_seq, there - n_seq, there)

    smalls = [pltpu.make_async_copy(a, b, small_sem.at[i]) for i, (a, b) in enumerate(
        ((lengths_hbm, lengths), (map_hbm, block_map), (q_hbm, q_ref)))]

    def load(half, which, piece):
        owner = jnp.where(half == 0, head, mate)
        source, target = ((k_hbm, k_buf), (v_hbm, v_buf))[which]
        lanes = pl.ds(pl.multiple_of(owner * width, width), width)
        blocks = pl.ds(0, slots) if piece is None else pl.ds(piece * per, per)
        return pltpu.make_async_copy(
            source.at[:, blocks, :, lanes], target.at[half, :, blocks],
            kv_sem.at[half * 2 + which if piece is None else 2 * n_head + piece],
        )

    for copy in smalls:
        copy.start()
    for piece in range(pieces):
        load(0, 0, piece).start()
    load(1, 0, None).start(priority=1)
    load(0, 1, None).start(priority=1)

    barrier = pltpu.get_barrier_semaphore()
    lead = head == n_head - 1

    def q_copy():
        return pltpu.make_async_remote_copy(
            src_ref=q_ref, dst_ref=q_mate, send_sem=q_sem.at[0], recv_sem=q_sem.at[1],
            device_id={"head": mate}, device_id_type=MESH,
        )

    def tell_mate():
        pl.semaphore_signal(ready_sem, inc=1, device_id={"head": mate}, device_id_type=MESH)

    @pl.when(lead)
    def _():
        pl.semaphore_signal(barrier, inc=1, device_id={"head": mate}, device_id_type=MESH)
        pl.semaphore_wait(ready_sem, 1)

        def greet(d):
            pl.semaphore_signal(barrier, inc=1, device_id={"seq": turned(d)}, device_id_type=MESH)

        loop(1, n_seq, greet)

    @pl.when(jnp.logical_not(lead))
    def _():
        pl.semaphore_wait(barrier, 1)
        tell_mate()

    smalls[2].wait()
    q_copy().start()

    def everyone_in():
        @pl.when(lead)
        def _():
            pl.semaphore_wait(barrier, n_seq - 1)
            tell_mate()

        @pl.when(jnp.logical_not(lead))
        def _():
            pl.semaphore_wait(ready_sem, 1)

    def bias_of(b):
        parts = []
        for j in range(slots):
            here = block_map[b, me * slots + j] * BLK < lengths[b]
            parts.append(jnp.broadcast_to(jnp.where(here, 0.0, NEG), (rows_b, BLK)))
        return jnp.concatenate(parts, axis=1)

    def diagonal(q):
        lifted = q.astype(jnp.float32).reshape(rows, HD)
        wide = jnp.concatenate([lifted] * groups, axis=1)
        row_group = lax.rem(lax.broadcasted_iota(jnp.int32, wide.shape, 0), rows_b) // REP
        lane_group = lax.broadcasted_iota(jnp.int32, wide.shape, 1) // HD
        return jnp.where(row_group == lane_group, wide, 0.0).astype(jnp.bfloat16)

    for copy in smalls[:2]:
        copy.wait()
    load(1, 1, None).start(priority=1)
    bias = [bias_of(b) for b in range(batch)]

    def copies(half, d):
        where = {"seq": turned(d), "head": mate if half else head}
        return (
            pltpu.make_async_remote_copy(
                src_ref=stat_send.at[pl.ds(half, 1)], dst_ref=stat_recv.at[pl.ds(me, 1)],
                send_sem=ssend_sem, recv_sem=srecv_sem, device_id=where, device_id_type=MESH,
            ),
            pltpu.make_async_remote_copy(
                src_ref=num_send.at[half], dst_ref=num_recv.at[me],
                send_sem=nsend_sem, recv_sem=nrecv_sem, device_id=where, device_id_type=MESH,
            ),
        )

    def send(half, which, turns):
        if isinstance(turns, list):
            for d in turns:
                copies(half, d)[which].start()
        else:
            loop(*turns, lambda d: copies(half, d)[which].start())

    row_group = lax.broadcasted_iota(jnp.int32, (rows_b, HD), 0) // REP

    def multiply(acc, b, lhs, rhs, transpose):
        register = turn[b % 2]
        turn[b % 2] = 1 - register
        pltpu.matmul_push_rhs(rhs, register, b % 2, transpose=transpose)
        pltpu.matmul_acc_lhs(acc, lhs, load_staged_rhs=register)

    turn = [0, 0]

    def score(half, spread, t):
        for c in range(strips):
            for b in range(batch):
                keys = k_buf[half, b, t * per:(t + 1) * per, :, c * TILE:(c + 1) * TILE]
                multiply(
                    score_acc[half][b][t], b, spread[b * rows_b:(b + 1) * rows_b, c * TILE:(c + 1) * TILE],
                    keys.reshape(TILE, TILE), True,
                )

    def soften(half):
        expos, tops, totals = [], [], []
        for b in range(batch):
            raw = jnp.concatenate([pltpu.matmul_pop(acc) for acc in score_acc[half][b]], axis=1)
            scores = raw * (LOG2E / HD**0.5) + bias[b]
            top = jnp.max(scores, axis=1, keepdims=True)
            expo = jnp.exp2(scores - top)
            tops.append(top)
            totals.append(jnp.sum(expo, axis=1, keepdims=True))
            expos.append(expo.astype(jnp.bfloat16))
        column = jnp.concatenate(tops + totals + [jnp.zeros((HD - 2 * rows, 1), jnp.float32)], axis=0)
        stat_send[half:half + 1] = jnp.transpose(jnp.broadcast_to(column, (HD, HD)))[0:1]
        return expos

    def weigh(half, expos):
        for t in range(pieces):
            for c in range(strips):
                for b in range(batch):
                    values = v_buf[half, b, t * per:(t + 1) * per, :, c * TILE:(c + 1) * TILE]
                    multiply(
                        value_acc[half][b][c], b, expos[b][:, t * TILE:(t + 1) * TILE],
                        values.reshape(TILE, TILE), False,
                    )

    def finish(half):
        nums = []
        for b in range(batch):
            part = jnp.zeros((rows_b, HD), jnp.float32)
            for c in range(strips):
                full = pltpu.matmul_pop(value_acc[half][b][c])
                for g in range(TILE // HD):
                    part = jnp.where(row_group == c * (TILE // HD) + g, full[:, g * HD:(g + 1) * HD], part)
            nums.append(part)
        num_send[half] = jnp.concatenate(nums, axis=0).astype(jnp.bfloat16)

    own_turns, mate_turns = (1, n_seq), (0, n_seq)
    if small:
        own_turns, mate_turns = list(range(n_seq - 1, 0, -1)), list(range(n_seq - 1, -1, -1))
    spread = diagonal(q_ref[...])
    for t in range(pieces):
        load(0, 0, t).wait()
        score(0, spread, t)
    q_copy().wait()
    spread = diagonal(q_mate[...])
    load(1, 0, None).wait()
    for t in range(pieces):
        score(1, spread, t)
    expos = soften(0)
    everyone_in()
    send(0, 0, own_turns)
    load(0, 1, None).wait()
    weigh(0, expos)
    expos = soften(1)
    send(1, 0, mate_turns)
    load(1, 1, None).wait()
    weigh(1, expos)
    finish(0)
    send(0, 1, own_turns)
    finish(1)
    send(1, 1, mate_turns)

    all_nums = pltpu.make_async_remote_copy(
        src_ref=num_recv.at[pl.ds(0, n_all - 1)], dst_ref=num_recv.at[pl.ds(0, n_all - 1)],
        send_sem=nsend_sem, recv_sem=nrecv_sem, device_id={"head": mate}, device_id_type=MESH,
    )
    all_stats = pltpu.make_async_remote_copy(
        src_ref=stat_recv.at[pl.ds(0, n_all - 1)], dst_ref=stat_recv.at[pl.ds(0, n_all - 1)],
        send_sem=ssend_sem, recv_sem=srecv_sem, device_id={"head": mate}, device_id_type=MESH,
    )
    all_stats.wait_send()
    all_nums.wait_send()
    stat_recv[pl.ds(me, 1)] = stat_send[0:1]
    num_recv[me] = num_send[0]
    all_stats.wait_recv()
    stats = stat_recv[...]
    top = stats[:, :rows]
    total = stats[:, rows:2 * rows]
    factor = jnp.exp2(top - jnp.max(top, axis=0, keepdims=True))
    share = factor / jnp.sum(factor * total, axis=0, keepdims=True)
    share_columns = jnp.transpose(jnp.concatenate(
        [share, jnp.zeros((n_all, HD - rows), jnp.float32)], axis=1))[:rows]
    for s in range(n_all):
        share_ref[s] = jnp.broadcast_to(share_columns[:, s:s + 1], (rows, HD))
    all_nums.wait_recv()

    def term(s):
        return share_ref[s] * num_recv[s].astype(jnp.float32)

    if small:
        terms = [term(s) for s in range(n_all)]
        while len(terms) > 1:
            terms = [a + b for a, b in zip(terms[::2], terms[1::2])] + terms[len(terms) // 2 * 2:]
        result = terms[0]
    else:
        result = lax.fori_loop(0, n_all, lambda s, acc: acc + term(s), jnp.zeros((rows, HD), jnp.float32))
    for b in range(batch):
        order_ref[pl.ds(b, rows_b, stride=batch), :] = result[b * rows_b:(b + 1) * rows_b]
    out_ref[...] = order_ref[...].astype(out_ref.dtype)


def with_accumulators(n_seq, n_head, *refs):
    batch, slots = refs[3].shape[0], refs[3].shape[1]
    width = refs[3].shape[3] // n_head
    rows_b = width // HD * REP

    def accumulators(count):
        return [[[pltpu.ACC(b % 2)((rows_b, TILE), jnp.float32) for _ in range(count)]
                 for b in range(batch)] for _ in range(n_head)]

    pl.run_scoped(
        lambda score_acc, value_acc: kernel(n_seq, n_head, score_acc, value_acc, *refs),
        accumulators(slots * BLK // TILE), accumulators(width // TILE),
    )


def solution(mesh):
    n_seq, n_head = mesh.shape["seq"], mesh.shape["head"]
    n_all = n_seq * n_head

    def on_device(key_cache, value_cache, query, lengths, block_map):
        batch, slots, _, channels = key_cache.shape
        width = channels // n_head
        rows_b = (width // HD) * REP
        rows = batch * rows_b
        dma = pltpu.SemaphoreType.DMA
        result = pl.pallas_call(
            functools.partial(with_accumulators, n_seq, n_head),
            out_shape=pltpu.VMEM((rows, HD), jnp.bfloat16),
            in_specs=[
                *[pl.BlockSpec(memory_space=pl.ANY)] * 5,
            ],
            out_specs=pl.BlockSpec(memory_space=pltpu.VMEM),
            scratch_shapes=[
                pltpu.SMEM(lengths.shape, jnp.int32),
                pltpu.SMEM(block_map.shape, jnp.int32),
                pltpu.VMEM(query.shape, jnp.bfloat16),
                dma((3,)),
                pltpu.VMEM((n_head, batch, slots, BLK, width), jnp.bfloat16),
                pltpu.VMEM((n_head, batch, slots, BLK, width), jnp.bfloat16),
                pltpu.VMEM(query.shape, jnp.bfloat16),
                pltpu.VMEM((n_head, rows, HD), jnp.bfloat16),
                pltpu.VMEM((n_head, HD), jnp.float32),
                pltpu.VMEM((n_all, rows, HD), jnp.bfloat16),
                pltpu.VMEM((n_all, HD), jnp.float32),
                pltpu.VMEM((n_all, rows, HD), jnp.float32),
                pltpu.VMEM((rows, HD), jnp.float32),
                dma((2 * n_head + slots * BLK // TILE,)),
                dma((2,)),
                dma(()),
                dma(()),
                dma(()),
                dma(()),
                pltpu.SemaphoreType.REGULAR,
            ],
            compiler_params=pltpu.CompilerParams(collective_id=0, has_side_effects=True),
        )(lengths, block_map, query, key_cache, value_cache)
        return result.reshape(rows_b, batch, HD).transpose(1, 0, 2).reshape(batch, rows_b * HD)

    placed = (
        P("grp", ("seq", "head"), None, None),
        P("grp", ("seq", "head"), None, None),
        P("grp", "head"),
        P("grp"),
        P("grp", None),
    )
    return jax.shard_map(
        on_device, mesh=mesh, in_specs=placed, out_specs=P("grp", "head"), check_vma=False
    )
```

```python
import functools

import jax
import jax.numpy as jnp
from jax import lax
from jax.experimental import pallas as pl
from jax.experimental.pallas import tpu as pltpu
from jax.sharding import PartitionSpec as P

QH = 32
KVH = 8
HD = 128
BLK = 128
TILE = 256
REP = QH // KVH
MESH = pl.DeviceIdType.MESH
NEG = -1e30
LOG2E = 1.4426950408889634


def kernel(
    n_seq, n_head, score_acc, value_acc,
    lengths_hbm, map_hbm, q_hbm, k_hbm, v_hbm, out_ref,
    lengths, block_map, q_ref, small_sem,
    k_buf, v_buf, q_mate, num_send, stat_send, num_recv, stat_recv, share_ref, order_ref,
    kv_sem, q_sem, nsend_sem, nrecv_sem, ssend_sem, srecv_sem, ready_sem,
):
    seq = lax.axis_index("seq")
    head = lax.axis_index("head")
    batch, slots = k_hbm.shape[0], k_hbm.shape[1]
    width = k_hbm.shape[3] // n_head
    groups = width // HD
    rows_b = groups * REP
    rows = batch * rows_b
    tokens = slots * BLK
    per = TILE // BLK
    pieces = tokens // TILE
    strips = width // TILE
    me = seq * n_head + head
    mate = n_head - 1 - head
    n_all = n_seq * n_head
    small = n_all <= 16

    def loop(lo, hi, body):
        if small:
            for i in range(lo, hi):
                body(i)
        else:
            def step(i, carry):
                body(i)
                return carry
            lax.fori_loop(lo, hi, step, 0)

    def turned(d):
        return jnp.where(d == n_seq - 1, seq, d + jnp.where(d >= seq, 1, 0))

    smalls = [pltpu.make_async_copy(a, b, small_sem.at[i]) for i, (a, b) in enumerate(
        ((lengths_hbm, lengths), (map_hbm, block_map), (q_hbm, q_ref)))]

    def load(half, which, piece=None):
        owner = jnp.where(half == 0, head, mate)
        source, target = ((k_hbm, k_buf), (v_hbm, v_buf))[which]
        lanes = pl.ds(pl.multiple_of(owner * width, width), width)
        blocks = pl.ds(0, slots) if piece is None else pl.ds(piece * per, per)
        return pltpu.make_async_copy(
            source.at[:, blocks, :, lanes], target.at[half, :, blocks],
            kv_sem.at[half * (pieces + 1) + (pieces if piece is None else piece)],
        )

    for copy in smalls:
        copy.start()
    for piece in range(pieces):
        load(0, 0, piece).start()
    load(0, 1).start(priority=1)

    barrier = pltpu.get_barrier_semaphore()
    lead = head == n_head - 1

    def q_copy():
        return pltpu.make_async_remote_copy(
            src_ref=q_ref, dst_ref=q_mate, send_sem=q_sem.at[0], recv_sem=q_sem.at[1],
            device_id={"head": mate}, device_id_type=MESH,
        )

    def tell_mate():
        pl.semaphore_signal(ready_sem, inc=1, device_id={"head": mate}, device_id_type=MESH)

    @pl.when(lead)
    def _():
        pl.semaphore_signal(barrier, inc=1, device_id={"head": mate}, device_id_type=MESH)
        pl.semaphore_wait(ready_sem, 1)

        def greet(d):
            pl.semaphore_signal(barrier, inc=1, device_id={"seq": turned(d)}, device_id_type=MESH)

        loop(0, n_seq - 1, greet)

    @pl.when(jnp.logical_not(lead))
    def _():
        pl.semaphore_wait(barrier, 1)
        tell_mate()

    smalls[2].wait()
    q_copy().start()

    def everyone_in():
        @pl.when(lead)
        def _():
            pl.semaphore_wait(barrier, n_seq - 1)
            tell_mate()

        @pl.when(jnp.logical_not(lead))
        def _():
            pl.semaphore_wait(ready_sem, 1)

    def bias_of(b):
        parts = []
        for j in range(slots):
            here = block_map[b, me * slots + j] * BLK < lengths[b]
            parts.append(jnp.broadcast_to(jnp.where(here, 0.0, NEG), (rows_b, BLK)))
        return jnp.concatenate(parts, axis=1)

    def diagonal(q):
        lifted = q.astype(jnp.float32).reshape(rows, HD)
        wide = jnp.concatenate([lifted] * groups, axis=1)
        row_group = lax.rem(lax.broadcasted_iota(jnp.int32, wide.shape, 0), rows_b) // REP
        lane_group = lax.broadcasted_iota(jnp.int32, wide.shape, 1) // HD
        return jnp.where(row_group == lane_group, wide, 0.0).astype(jnp.bfloat16)

    for copy in smalls[:2]:
        copy.wait()
    for piece in range(pieces):
        load(1, 0, piece).start()
    load(1, 1).start(priority=1)
    bias = [bias_of(b) for b in range(batch)]

    def copies(half, d):
        where = {"seq": turned(d), "head": mate if half else head}
        return (
            pltpu.make_async_remote_copy(
                src_ref=stat_send.at[pl.ds(half, 1)], dst_ref=stat_recv.at[pl.ds(me, 1)],
                send_sem=ssend_sem, recv_sem=srecv_sem, device_id=where, device_id_type=MESH,
            ),
            pltpu.make_async_remote_copy(
                src_ref=num_send.at[half], dst_ref=num_recv.at[me],
                send_sem=nsend_sem, recv_sem=nrecv_sem, device_id=where, device_id_type=MESH,
            ),
        )

    def send(half, which, turns):
        loop(*turns, lambda d: copies(half, d)[which].start())

    row_group = lax.broadcasted_iota(jnp.int32, (rows_b, HD), 0) // REP

    def multiply(acc, b, lhs, rhs, transpose):
        register = turn[b % 2]
        turn[b % 2] = 1 - register
        pltpu.matmul_push_rhs(rhs, register, b % 2, transpose=transpose)
        pltpu.matmul_acc_lhs(acc, lhs, load_staged_rhs=register)

    turn = [0, 0]

    def score(half, spread, t):
        for c in range(strips):
            for b in range(batch):
                keys = k_buf[half, b, t * per:(t + 1) * per, :, c * TILE:(c + 1) * TILE]
                multiply(
                    score_acc[half][b][t], b, spread[b * rows_b:(b + 1) * rows_b, c * TILE:(c + 1) * TILE],
                    keys.reshape(TILE, TILE), True,
                )

    def soften(half):
        expos, tops, totals = [], [], []
        for b in range(batch):
            raw = jnp.concatenate([pltpu.matmul_pop(acc) for acc in score_acc[half][b]], axis=1)
            scores = raw * (LOG2E / HD**0.5) + bias[b]
            top = jnp.max(scores, axis=1, keepdims=True)
            expo = jnp.exp2(scores - top)
            tops.append(top)
            totals.append(jnp.sum(expo, axis=1, keepdims=True))
            expos.append(expo.astype(jnp.bfloat16))
        column = jnp.concatenate(tops + totals + [jnp.zeros((HD - 2 * rows, 1), jnp.float32)], axis=0)
        stat_send[half:half + 1] = jnp.transpose(jnp.broadcast_to(column, (HD, HD)))[0:1]
        return expos

    def weigh(half, expos):
        for t in range(pieces):
            for c in range(strips):
                for b in range(batch):
                    values = v_buf[half, b, t * per:(t + 1) * per, :, c * TILE:(c + 1) * TILE]
                    multiply(
                        value_acc[half][b][c], b, expos[b][:, t * TILE:(t + 1) * TILE],
                        values.reshape(TILE, TILE), False,
                    )

    def finish(half):
        nums = []
        for b in range(batch):
            part = jnp.zeros((rows_b, HD), jnp.float32)
            for c in range(strips):
                full = pltpu.matmul_pop(value_acc[half][b][c])
                for g in range(TILE // HD):
                    part = jnp.where(row_group == c * (TILE // HD) + g, full[:, g * HD:(g + 1) * HD], part)
            nums.append(part)
        num_send[half] = jnp.concatenate(nums, axis=0).astype(jnp.bfloat16)

    own_turns, mate_turns, first = (0, n_seq - 1), (0, n_seq), max(1, n_seq // 4)
    spread = diagonal(q_ref[...])
    for t in range(pieces):
        load(0, 0, t).wait()
        score(0, spread, t)
    expos = soften(0)
    everyone_in()
    send(0, 0, own_turns)
    load(0, 1).wait()
    weigh(0, expos)
    q_copy().wait()
    spread = diagonal(q_mate[...])
    for t in range(0, 1):
        load(1, 0, t).wait()
        score(1, spread, t)
    finish(0)
    send(0, 1, (0, first))
    for t in range(1, pieces):
        load(1, 0, t).wait()
        score(1, spread, t)
    expos = soften(1)
    send(1, 0, mate_turns)
    load(1, 1).wait()
    weigh(1, expos)
    finish(1)
    send(1, 1, (0, first))
    send(0, 1, (first, n_seq - 1))
    send(1, 1, (first, n_seq))

    all_nums = pltpu.make_async_remote_copy(
        src_ref=num_recv.at[pl.ds(0, n_all - 1)], dst_ref=num_recv.at[pl.ds(0, n_all - 1)],
        send_sem=nsend_sem, recv_sem=nrecv_sem, device_id={"head": mate}, device_id_type=MESH,
    )
    all_stats = pltpu.make_async_remote_copy(
        src_ref=stat_recv.at[pl.ds(0, n_all - 1)], dst_ref=stat_recv.at[pl.ds(0, n_all - 1)],
        send_sem=ssend_sem, recv_sem=srecv_sem, device_id={"head": mate}, device_id_type=MESH,
    )
    all_stats.wait_send()
    all_nums.wait_send()
    stat_recv[pl.ds(me, 1)] = stat_send[0:1]
    num_recv[me] = num_send[0]
    all_stats.wait_recv()
    stats = stat_recv[...]
    top = stats[:, :rows]
    total = stats[:, rows:2 * rows]
    factor = jnp.exp2(top - jnp.max(top, axis=0, keepdims=True))
    share = factor / jnp.sum(factor * total, axis=0, keepdims=True)
    share_columns = jnp.transpose(jnp.concatenate(
        [share, jnp.zeros((n_all, HD - rows), jnp.float32)], axis=1))[:rows]
    for s in range(n_all):
        share_ref[s] = jnp.broadcast_to(share_columns[:, s:s + 1], (rows, HD))
    all_nums.wait_recv()

    def term(s):
        return share_ref[s] * num_recv[s].astype(jnp.float32)

    if small:
        terms = [term(s) for s in range(n_all)]
        while len(terms) > 1:
            terms = [a + b for a, b in zip(terms[::2], terms[1::2])] + terms[len(terms) // 2 * 2:]
        result = terms[0]
    else:
        result = lax.fori_loop(0, n_all, lambda s, acc: acc + term(s), jnp.zeros((rows, HD), jnp.float32))
    for b in range(batch):
        order_ref[pl.ds(b, rows_b, stride=batch), :] = result[b * rows_b:(b + 1) * rows_b]
    out_ref[...] = order_ref[...].astype(out_ref.dtype)


def with_accumulators(n_seq, n_head, *refs):
    batch, slots = refs[3].shape[0], refs[3].shape[1]
    width = refs[3].shape[3] // n_head
    rows_b = width // HD * REP

    def accumulators(count):
        return [[[pltpu.ACC(b % 2)((rows_b, TILE), jnp.float32) for _ in range(count)]
                 for b in range(batch)] for _ in range(n_head)]

    pl.run_scoped(
        lambda score_acc, value_acc: kernel(n_seq, n_head, score_acc, value_acc, *refs),
        accumulators(slots * BLK // TILE), accumulators(width // TILE),
    )


def solution(mesh):
    n_seq, n_head = mesh.shape["seq"], mesh.shape["head"]
    n_all = n_seq * n_head

    def on_device(key_cache, value_cache, query, lengths, block_map):
        batch, slots, _, channels = key_cache.shape
        width = channels // n_head
        rows_b = (width // HD) * REP
        rows = batch * rows_b
        dma = pltpu.SemaphoreType.DMA
        result = pl.pallas_call(
            functools.partial(with_accumulators, n_seq, n_head),
            out_shape=pltpu.VMEM((rows, HD), jnp.bfloat16),
            in_specs=[
                *[pl.BlockSpec(memory_space=pl.ANY)] * 5,
            ],
            out_specs=pl.BlockSpec(memory_space=pltpu.VMEM),
            scratch_shapes=[
                pltpu.SMEM(lengths.shape, jnp.int32),
                pltpu.SMEM(block_map.shape, jnp.int32),
                pltpu.VMEM(query.shape, jnp.bfloat16),
                dma((3,)),
                pltpu.VMEM((n_head, batch, slots, BLK, width), jnp.bfloat16),
                pltpu.VMEM((n_head, batch, slots, BLK, width), jnp.bfloat16),
                pltpu.VMEM(query.shape, jnp.bfloat16),
                pltpu.VMEM((n_head, rows, HD), jnp.bfloat16),
                pltpu.VMEM((n_head, HD), jnp.float32),
                pltpu.VMEM((n_all, rows, HD), jnp.bfloat16),
                pltpu.VMEM((n_all, HD), jnp.float32),
                pltpu.VMEM((n_all, rows, HD), jnp.float32),
                pltpu.VMEM((rows, HD), jnp.float32),
                dma((n_head * (slots * BLK // TILE + 1),)),
                dma((2,)),
                dma(()),
                dma(()),
                dma(()),
                dma(()),
                pltpu.SemaphoreType.REGULAR,
            ],
            compiler_params=pltpu.CompilerParams(collective_id=0, has_side_effects=True),
        )(lengths, block_map, query, key_cache, value_cache)
        return result.reshape(rows_b, batch, HD).transpose(1, 0, 2).reshape(batch, rows_b * HD)

    placed = (
        P("grp", ("seq", "head"), None, None),
        P("grp", ("seq", "head"), None, None),
        P("grp", "head"),
        P("grp"),
        P("grp", None),
    )
    return jax.shard_map(
        on_device, mesh=mesh, in_specs=placed, out_specs=P("grp", "head"), check_vma=False
    )
```

```python
import functools

import jax
import jax.numpy as jnp
from jax import lax
from jax.experimental import pallas as pl
from jax.experimental.pallas import tpu as pltpu
from jax.sharding import PartitionSpec as P

QH = 32
KVH = 8
HD = 128
BLK = 128
TILE = 256
REP = QH // KVH
MESH = pl.DeviceIdType.MESH
NEG = -1e30
LOG2E = 1.4426950408889634


def kernel(
    n_seq, n_head, score_acc, value_acc, small_sem, kv_sem, qsend_sem, nsend_sem, ssend_sem,
    lengths_hbm, map_hbm, q_hbm, k_hbm, v_hbm, out_ref,
    lengths, block_map, q_ref,
    k_buf, v_buf, q_mate, num_send, stat_send, num_recv, stat_recv, share_ref, order_ref,
    q_sem, nrecv_sem, srecv_sem, ready_sem,
):
    seq = lax.axis_index("seq")
    head = lax.axis_index("head")
    batch, slots = k_hbm.shape[0], k_hbm.shape[1]
    width = k_hbm.shape[3] // n_head
    groups = width // HD
    rows_b = groups * REP
    rows = batch * rows_b
    tokens = slots * BLK
    per = TILE // BLK
    pieces = tokens // TILE
    strips = width // TILE
    me = seq * n_head + head
    mate = n_head - 1 - head
    n_all = n_seq * n_head
    small = n_all <= 16

    def loop(lo, hi, body):
        if small:
            for i in range(lo, hi):
                body(i)
        else:
            def step(i, carry):
                body(i)
                return carry
            lax.fori_loop(lo, hi, step, 0)

    def turned(d):
        return jnp.where(d == n_seq - 1, seq, d + jnp.where(d >= seq, 1, 0))

    smalls = [pltpu.make_async_copy(a, b, small_sem.at[i]) for i, (a, b) in enumerate(
        ((lengths_hbm, lengths), (map_hbm, block_map), (q_hbm, q_ref)))]

    def load(half, which, piece=None):
        owner = jnp.where(half == 0, head, mate)
        source, target = ((k_hbm, k_buf), (v_hbm, v_buf))[which]
        lanes = pl.ds(pl.multiple_of(owner * width, width), width)
        blocks = pl.ds(0, slots) if piece is None else pl.ds(piece * per, per)
        return pltpu.make_async_copy(
            source.at[:, blocks, :, lanes], target.at[half, :, blocks],
            kv_sem.at[half * (pieces + 1) + (pieces if piece is None else piece)],
        )

    for copy in smalls:
        copy.start()
    for piece in range(pieces):
        load(0, 0, piece).start()
    load(0, 1).start(priority=1)

    barrier = pltpu.get_barrier_semaphore()
    lead = head == n_head - 1

    def q_copy():
        return pltpu.make_async_remote_copy(
            src_ref=q_ref, dst_ref=q_mate, send_sem=qsend_sem, recv_sem=q_sem,
            device_id={"head": mate}, device_id_type=MESH,
        )

    def tell_mate():
        pl.semaphore_signal(ready_sem, inc=1, device_id={"head": mate}, device_id_type=MESH)

    @pl.when(lead)
    def _():
        pl.semaphore_signal(barrier, inc=1, device_id={"head": mate}, device_id_type=MESH)
        pl.semaphore_wait(ready_sem, 1)

        def greet(d):
            pl.semaphore_signal(barrier, inc=1, device_id={"seq": turned(d)}, device_id_type=MESH)

        loop(0, n_seq - 1, greet)

    @pl.when(jnp.logical_not(lead))
    def _():
        pl.semaphore_wait(barrier, 1)
        tell_mate()

    smalls[2].wait()
    q_copy().start()

    def everyone_in():
        @pl.when(lead)
        def _():
            pl.semaphore_wait(barrier, n_seq - 1)
            tell_mate()

        @pl.when(jnp.logical_not(lead))
        def _():
            pl.semaphore_wait(ready_sem, 1)

    def bias_of(b):
        parts = []
        for j in range(slots):
            here = block_map[b, me * slots + j] * BLK < lengths[b]
            parts.append(jnp.broadcast_to(jnp.where(here, 0.0, NEG), (rows_b, BLK)))
        return jnp.concatenate(parts, axis=1)

    def diagonal(q):
        lifted = q.astype(jnp.float32).reshape(rows, HD)
        wide = jnp.concatenate([lifted] * groups, axis=1)
        row_group = lax.rem(lax.broadcasted_iota(jnp.int32, wide.shape, 0), rows_b) // REP
        lane_group = lax.broadcasted_iota(jnp.int32, wide.shape, 1) // HD
        return jnp.where(row_group == lane_group, wide, 0.0).astype(jnp.bfloat16)

    for copy in smalls[:2]:
        copy.wait()
    for piece in range(pieces):
        load(1, 0, piece).start()
    load(1, 1).start(priority=1)
    bias = [bias_of(b) for b in range(batch)]

    def copies(half, d):
        where = {"seq": turned(d), "head": mate if half else head}
        return (
            pltpu.make_async_remote_copy(
                src_ref=stat_send.at[pl.ds(half, 1)], dst_ref=stat_recv.at[pl.ds(me, 1)],
                send_sem=ssend_sem, recv_sem=srecv_sem, device_id=where, device_id_type=MESH,
            ),
            pltpu.make_async_remote_copy(
                src_ref=num_send.at[half], dst_ref=num_recv.at[me],
                send_sem=nsend_sem, recv_sem=nrecv_sem, device_id=where, device_id_type=MESH,
            ),
        )

    def send(half, which, turns):
        loop(*turns, lambda d: copies(half, d)[which].start())

    row_group = lax.broadcasted_iota(jnp.int32, (rows_b, HD), 0) // REP
    row = lax.broadcasted_iota(jnp.int32, (rows, HD), 0)
    lane = lax.broadcasted_iota(jnp.int32, (rows, HD), 1)

    def multiply(acc, b, lhs, rhs, transpose):
        register = turn[b % 2]
        turn[b % 2] = 1 - register
        pltpu.matmul_push_rhs(rhs, register, b % 2, transpose=transpose)
        pltpu.matmul_acc_lhs(acc, lhs, load_staged_rhs=register)

    turn = [0, 0]

    def score(half, spread, t):
        for c in range(strips):
            for b in range(batch):
                keys = k_buf[half, b, t * per:(t + 1) * per, :, c * TILE:(c + 1) * TILE]
                multiply(
                    score_acc[half][b][t], b, spread[b * rows_b:(b + 1) * rows_b, c * TILE:(c + 1) * TILE],
                    keys.reshape(TILE, TILE), True,
                )

    def soften(half):
        expos, tops, totals = [], [], []
        for b in range(batch):
            raw = jnp.concatenate([pltpu.matmul_pop(acc) for acc in score_acc[half][b]], axis=1)
            scores = raw * (LOG2E / HD**0.5) + bias[b]
            top = jnp.max(scores, axis=1, keepdims=True)
            expo = jnp.exp2(scores - top)
            tops.append(top)
            totals.append(jnp.sum(expo, axis=1, keepdims=True))
            expos.append(expo.astype(jnp.bfloat16))
        record = jnp.where(lane == row, jnp.concatenate(tops, axis=0), 0.0)
        record = jnp.where(lane == row + rows, jnp.concatenate(totals, axis=0), record)
        stat_send[half:half + 1] = jnp.sum(record, axis=0, keepdims=True)
        return expos

    def weigh(half, expos):
        for t in range(pieces):
            for c in range(strips):
                for b in range(batch):
                    values = v_buf[half, b, t * per:(t + 1) * per, :, c * TILE:(c + 1) * TILE]
                    multiply(
                        value_acc[half][b][c], b, expos[b][:, t * TILE:(t + 1) * TILE],
                        values.reshape(TILE, TILE), False,
                    )

    def finish(half):
        nums = []
        for b in range(batch):
            part = jnp.zeros((rows_b, HD), jnp.float32)
            for c in range(strips):
                full = pltpu.matmul_pop(value_acc[half][b][c])
                for g in range(TILE // HD):
                    part = jnp.where(row_group == c * (TILE // HD) + g, full[:, g * HD:(g + 1) * HD], part)
            nums.append(part)
        num_send[half] = jnp.concatenate(nums, axis=0).astype(jnp.bfloat16)

    own_turns, mate_turns, first = (0, n_seq - 1), (0, n_seq), max(1, n_seq // 4)
    spread = diagonal(q_ref[...])
    for t in range(pieces):
        load(0, 0, t).wait()
        score(0, spread, t)
    expos = soften(0)
    everyone_in()
    send(0, 0, own_turns)
    load(0, 1).wait()
    weigh(0, expos)
    q_copy().wait()
    spread = diagonal(q_mate[...])
    for t in range(0, 1):
        load(1, 0, t).wait()
        score(1, spread, t)
    finish(0)
    send(0, 1, (0, first))
    for t in range(1, pieces):
        load(1, 0, t).wait()
        score(1, spread, t)
    expos = soften(1)
    send(1, 0, mate_turns)
    load(1, 1).wait()
    weigh(1, expos)
    finish(1)
    send(1, 1, (0, first))
    send(0, 1, (first, n_seq - 1))
    send(1, 1, (first, n_seq))

    all_nums = pltpu.make_async_remote_copy(
        src_ref=num_recv.at[pl.ds(0, n_all - 1)], dst_ref=num_recv.at[pl.ds(0, n_all - 1)],
        send_sem=nsend_sem, recv_sem=nrecv_sem, device_id={"head": mate}, device_id_type=MESH,
    )
    all_stats = pltpu.make_async_remote_copy(
        src_ref=stat_recv.at[pl.ds(0, n_all - 1)], dst_ref=stat_recv.at[pl.ds(0, n_all - 1)],
        send_sem=ssend_sem, recv_sem=srecv_sem, device_id={"head": mate}, device_id_type=MESH,
    )
    all_stats.wait_send()
    all_nums.wait_send()
    stat_recv[pl.ds(me, 1)] = stat_send[0:1]
    num_recv[me] = num_send[0]
    all_stats.wait_recv()
    stats = stat_recv[...]
    factor = jnp.exp2(stats - jnp.max(stats, axis=0, keepdims=True))

    def column(line):
        return jnp.sum(jnp.where(lane == row, line, 0.0), axis=1, keepdims=True)

    for s in range(n_all):
        share_ref[s] = jnp.broadcast_to(column(factor[s:s + 1]), (rows, HD))
    whole = jnp.sum(factor[:, :rows] * stats[:, rows:2 * rows], axis=0, keepdims=True)
    whole = jnp.concatenate([whole, jnp.ones((1, HD - rows), jnp.float32)], axis=1)
    scale = column(1.0 / whole)
    all_nums.wait_recv()

    def term(s):
        return share_ref[s] * num_recv[s].astype(jnp.float32)

    if small:
        terms = [term(s) for s in range(n_all)]
        while len(terms) > 1:
            terms = [a + b for a, b in zip(terms[::2], terms[1::2])] + terms[len(terms) // 2 * 2:]
        result = terms[0]
    else:
        result = lax.fori_loop(0, n_all, lambda s, acc: acc + term(s), jnp.zeros((rows, HD), jnp.float32))
    result = result * scale
    for b in range(batch):
        order_ref[pl.ds(b, rows_b, stride=batch), :] = result[b * rows_b:(b + 1) * rows_b]
    out_ref[...] = order_ref[...].astype(out_ref.dtype)


def with_accumulators(n_seq, n_head, *refs):
    batch, slots = refs[3].shape[0], refs[3].shape[1]
    width = refs[3].shape[3] // n_head
    rows_b = width // HD * REP
    dma = pltpu.SemaphoreType.DMA

    def accumulators(count):
        return [[[pltpu.ACC(b % 2)((rows_b, TILE), jnp.float32) for _ in range(count)]
                 for b in range(batch)] for _ in range(n_head)]

    pl.run_scoped(
        lambda *scoped: kernel(n_seq, n_head, *scoped, *refs),
        accumulators(slots * BLK // TILE), accumulators(width // TILE),
        dma((3,)), dma((n_head * (slots * BLK // TILE + 1),)), dma(()), dma(()), dma(()),
    )


def solution(mesh):
    n_seq, n_head = mesh.shape["seq"], mesh.shape["head"]
    n_all = n_seq * n_head

    def on_device(key_cache, value_cache, query, lengths, block_map):
        batch, slots, _, channels = key_cache.shape
        width = channels // n_head
        rows_b = (width // HD) * REP
        rows = batch * rows_b
        dma = pltpu.SemaphoreType.DMA
        result = pl.pallas_call(
            functools.partial(with_accumulators, n_seq, n_head),
            out_shape=pltpu.VMEM((rows, HD), jnp.bfloat16),
            in_specs=[
                *[pl.BlockSpec(memory_space=pl.ANY)] * 5,
            ],
            out_specs=pl.BlockSpec(memory_space=pltpu.VMEM),
            scratch_shapes=[
                pltpu.SMEM(lengths.shape, jnp.int32),
                pltpu.SMEM(block_map.shape, jnp.int32),
                pltpu.VMEM(query.shape, jnp.bfloat16),
                pltpu.VMEM((n_head, batch, slots, BLK, width), jnp.bfloat16),
                pltpu.VMEM((n_head, batch, slots, BLK, width), jnp.bfloat16),
                pltpu.VMEM(query.shape, jnp.bfloat16),
                pltpu.VMEM((n_head, rows, HD), jnp.bfloat16),
                pltpu.VMEM((n_head, HD), jnp.float32),
                pltpu.VMEM((n_all, rows, HD), jnp.bfloat16),
                pltpu.VMEM((n_all, HD), jnp.float32),
                pltpu.VMEM((n_all, rows, HD), jnp.float32),
                pltpu.VMEM((rows, HD), jnp.float32),
                dma(()),
                dma(()),
                dma(()),
                pltpu.SemaphoreType.REGULAR,
            ],
            compiler_params=pltpu.CompilerParams(collective_id=0, has_side_effects=True),
        )(lengths, block_map, query, key_cache, value_cache)
        return result.reshape(rows_b, batch, HD).transpose(1, 0, 2).reshape(batch, rows_b * HD)

    placed = (
        P("grp", ("seq", "head"), None, None),
        P("grp", ("seq", "head"), None, None),
        P("grp", "head"),
        P("grp"),
        P("grp", None),
    )
    return jax.shard_map(
        on_device, mesh=mesh, in_specs=placed, out_specs=P("grp", "head"), check_vma=False
    )
```

```python
import functools

import jax
import jax.numpy as jnp
from jax import lax
from jax.experimental import pallas as pl
from jax.experimental.pallas import tpu as pltpu
from jax.sharding import PartitionSpec as P

QH = 32
KVH = 8
HD = 128
BLK = 128
TILE = 256
REP = QH // KVH
MESH = pl.DeviceIdType.MESH
NEG = -1e30
LOG2E = 1.4426950408889634


def kernel(
    n_seq, n_head, score_acc, value_acc, small_sem, kv_sem, qsend_sem, nsend_sem, ssend_sem,
    lengths_hbm, map_hbm, q_hbm, k_hbm, v_hbm, out_ref,
    lengths, block_map, q_ref,
    k_buf, v_buf, q_mate, num_send, stat_send, num_recv, stat_recv, share_ref, order_ref,
    q_sem, nrecv_sem, srecv_sem, ready_sem,
):
    seq = lax.axis_index("seq")
    head = lax.axis_index("head")
    batch, slots = k_hbm.shape[0], k_hbm.shape[1]
    width = k_hbm.shape[3] // n_head
    groups = width // HD
    rows_b = groups * REP
    rows = batch * rows_b
    tokens = slots * BLK
    per = TILE // BLK
    pieces = tokens // TILE
    strips = width // TILE
    me = seq * n_head + head
    mate = n_head - 1 - head
    n_all = n_seq * n_head
    small = n_all <= 16

    def loop(lo, hi, body):
        if small:
            for i in range(lo, hi):
                body(i)
        else:
            def step(i, carry):
                body(i)
                return carry
            lax.fori_loop(lo, hi, step, 0)

    def turned(d):
        return jnp.where(d == n_seq - 1, seq, d + jnp.where(d >= seq, 1, 0))

    smalls = [pltpu.make_async_copy(a, b, small_sem.at[i]) for i, (a, b) in enumerate(
        ((lengths_hbm, lengths), (map_hbm, block_map), (q_hbm, q_ref)))]

    def load(half, which, piece=None):
        owner = jnp.where(half == 0, head, mate)
        source, target = ((k_hbm, k_buf), (v_hbm, v_buf))[which]
        lanes = pl.ds(pl.multiple_of(owner * width, width), width)
        blocks = pl.ds(0, slots) if piece is None else pl.ds(piece * per, per)
        return pltpu.make_async_copy(
            source.at[:, blocks, :, lanes], target.at[half, :, blocks],
            kv_sem.at[half * (pieces + 1) + (pieces if piece is None else piece)],
        )

    for copy in smalls:
        copy.start()
    for piece in range(pieces):
        load(0, 0, piece).start()
    load(0, 1).start(priority=1)

    barrier = pltpu.get_barrier_semaphore()
    lead = head == n_head - 1

    def q_copy():
        return pltpu.make_async_remote_copy(
            src_ref=q_ref, dst_ref=q_mate, send_sem=qsend_sem, recv_sem=q_sem,
            device_id={"head": mate}, device_id_type=MESH,
        )

    def tell_mate():
        pl.semaphore_signal(ready_sem, inc=1, device_id={"head": mate}, device_id_type=MESH)

    @pl.when(lead)
    def _():
        pl.semaphore_signal(barrier, inc=1, device_id={"head": mate}, device_id_type=MESH)
        pl.semaphore_wait(ready_sem, 1)

        def greet(d):
            pl.semaphore_signal(barrier, inc=1, device_id={"seq": turned(d)}, device_id_type=MESH)

        loop(0, n_seq - 1, greet)

    @pl.when(jnp.logical_not(lead))
    def _():
        pl.semaphore_wait(barrier, 1)
        tell_mate()

    smalls[2].wait()
    q_copy().start()

    def everyone_in():
        @pl.when(lead)
        def _():
            pl.semaphore_wait(barrier, n_seq - 1)
            tell_mate()

        @pl.when(jnp.logical_not(lead))
        def _():
            pl.semaphore_wait(ready_sem, 1)

    def bias_of(b):
        parts = []
        for j in range(slots):
            here = block_map[b, me * slots + j] * BLK < lengths[b]
            parts.append(jnp.broadcast_to(jnp.where(here, 0.0, NEG), (rows_b, BLK)))
        return jnp.concatenate(parts, axis=1)

    def diagonal(q):
        lifted = q.astype(jnp.float32).reshape(rows, HD)
        wide = jnp.concatenate([lifted] * groups, axis=1)
        row_group = lax.rem(lax.broadcasted_iota(jnp.int32, wide.shape, 0), rows_b) // REP
        lane_group = lax.broadcasted_iota(jnp.int32, wide.shape, 1) // HD
        return jnp.where(row_group == lane_group, wide, 0.0).astype(jnp.bfloat16)

    for copy in smalls[:2]:
        copy.wait()
    for piece in range(pieces):
        load(1, 0, piece).start()
    load(1, 1).start(priority=1)
    bias = [bias_of(b) for b in range(batch)]

    def copies(half, d):
        where = {"seq": turned(d), "head": mate if half else head}
        return (
            pltpu.make_async_remote_copy(
                src_ref=stat_send.at[pl.ds(half, 1)], dst_ref=stat_recv.at[pl.ds(me, 1)],
                send_sem=ssend_sem, recv_sem=srecv_sem, device_id=where, device_id_type=MESH,
            ),
            pltpu.make_async_remote_copy(
                src_ref=num_send.at[half], dst_ref=num_recv.at[me],
                send_sem=nsend_sem, recv_sem=nrecv_sem, device_id=where, device_id_type=MESH,
            ),
        )

    def send(half, which, turns):
        loop(*turns, lambda d: copies(half, d)[which].start())

    row_group = lax.broadcasted_iota(jnp.int32, (rows_b, HD), 0) // REP
    row = lax.broadcasted_iota(jnp.int32, (rows, HD), 0)
    lane = lax.broadcasted_iota(jnp.int32, (rows, HD), 1)

    def multiply(acc, b, lhs, rhs, transpose):
        register = turn[b % 2]
        turn[b % 2] = 1 - register
        pltpu.matmul_push_rhs(rhs, register, b % 2, transpose=transpose)
        pltpu.matmul_acc_lhs(acc, lhs, load_staged_rhs=register)

    turn = [0, 0]

    def score(half, spread, t):
        for c in range(strips):
            for b in range(batch):
                keys = k_buf[half, b, t * per:(t + 1) * per, :, c * TILE:(c + 1) * TILE]
                multiply(
                    score_acc[half][b][t], b, spread[b * rows_b:(b + 1) * rows_b, c * TILE:(c + 1) * TILE],
                    keys.reshape(TILE, TILE), True,
                )

    def soften(half):
        soft = []
        for b in range(batch):
            raw = jnp.concatenate([pltpu.matmul_pop(acc) for acc in score_acc[half][b]], axis=1)
            scores = raw * (LOG2E / HD**0.5) + bias[b]
            top = jnp.max(scores, axis=1, keepdims=True)
            soft.append((jnp.exp2(scores - top), top))
        return soft

    def note(half, soft):
        totals = [jnp.sum(expo, axis=1, keepdims=True) for expo, _ in soft]
        record = jnp.where(lane == row, jnp.concatenate([top for _, top in soft], axis=0), 0.0)
        record = jnp.where(lane == row + rows, jnp.concatenate(totals, axis=0), record)
        stat_send[half:half + 1] = jnp.sum(record, axis=0, keepdims=True)

    def weigh(half, soft):
        expos = [expo.astype(jnp.bfloat16) for expo, _ in soft]
        for t in range(pieces):
            for c in range(strips):
                for b in range(batch):
                    values = v_buf[half, b, t * per:(t + 1) * per, :, c * TILE:(c + 1) * TILE]
                    multiply(
                        value_acc[half][b][c], b, expos[b][:, t * TILE:(t + 1) * TILE],
                        values.reshape(TILE, TILE), False,
                    )

    def finish(half):
        nums = []
        for b in range(batch):
            part = jnp.zeros((rows_b, HD), jnp.float32)
            for c in range(strips):
                full = pltpu.matmul_pop(value_acc[half][b][c])
                for g in range(TILE // HD):
                    part = jnp.where(row_group == c * (TILE // HD) + g, full[:, g * HD:(g + 1) * HD], part)
            nums.append(part)
        num_send[half] = jnp.concatenate(nums, axis=0).astype(jnp.bfloat16)

    own_turns, mate_turns, first = (0, n_seq - 1), (0, n_seq), max(1, n_seq // 4)
    spread = diagonal(q_ref[...])
    for t in range(pieces):
        load(0, 0, t).wait()
        score(0, spread, t)
    soft = soften(0)
    load(0, 1).wait()
    weigh(0, soft)
    note(0, soft)
    everyone_in()
    send(0, 0, (0, first))
    q_copy().wait()
    spread = diagonal(q_mate[...])
    load(1, 0, 0).wait()
    score(1, spread, 0)
    finish(0)
    send(0, 1, (0, first))
    for t in range(1, pieces):
        load(1, 0, t).wait()
        score(1, spread, t)
    soft = soften(1)
    load(1, 1).wait()
    weigh(1, soft)
    note(1, soft)
    send(1, 0, (0, first))
    finish(1)
    send(1, 1, (0, first))
    send(0, 0, (first, n_seq - 1))
    send(1, 0, (first, n_seq))
    send(0, 1, (first, n_seq - 1))
    send(1, 1, (first, n_seq))

    all_nums = pltpu.make_async_remote_copy(
        src_ref=num_recv.at[pl.ds(0, n_all - 1)], dst_ref=num_recv.at[pl.ds(0, n_all - 1)],
        send_sem=nsend_sem, recv_sem=nrecv_sem, device_id={"head": mate}, device_id_type=MESH,
    )
    all_stats = pltpu.make_async_remote_copy(
        src_ref=stat_recv.at[pl.ds(0, n_all - 1)], dst_ref=stat_recv.at[pl.ds(0, n_all - 1)],
        send_sem=ssend_sem, recv_sem=srecv_sem, device_id={"head": mate}, device_id_type=MESH,
    )
    all_stats.wait_send()
    all_nums.wait_send()
    stat_recv[pl.ds(me, 1)] = stat_send[0:1]
    num_recv[me] = num_send[0]
    all_stats.wait_recv()
    stats = stat_recv[...]
    factor = jnp.exp2(stats - jnp.max(stats, axis=0, keepdims=True))

    def column(line):
        return jnp.sum(jnp.where(lane == row, line, 0.0), axis=1, keepdims=True)

    for s in range(n_all):
        share_ref[s] = jnp.broadcast_to(column(factor[s:s + 1]), (rows, HD))
    whole = jnp.sum(factor[:, :rows] * stats[:, rows:2 * rows], axis=0, keepdims=True)
    whole = jnp.concatenate([whole, jnp.ones((1, HD - rows), jnp.float32)], axis=1)
    scale = column(1.0 / whole)
    all_nums.wait_recv()

    def term(s):
        return share_ref[s] * num_recv[s].astype(jnp.float32)

    if small:
        terms = [term(s) for s in range(n_all)]
        while len(terms) > 1:
            terms = [a + b for a, b in zip(terms[::2], terms[1::2])] + terms[len(terms) // 2 * 2:]
        result = terms[0]
    else:
        result = lax.fori_loop(0, n_all, lambda s, acc: acc + term(s), jnp.zeros((rows, HD), jnp.float32))
    result = result * scale
    for b in range(batch):
        order_ref[pl.ds(b, rows_b, stride=batch), :] = result[b * rows_b:(b + 1) * rows_b]
    out_ref[...] = order_ref[...].astype(out_ref.dtype)


def with_accumulators(n_seq, n_head, *refs):
    batch, slots = refs[3].shape[0], refs[3].shape[1]
    width = refs[3].shape[3] // n_head
    rows_b = width // HD * REP
    dma = pltpu.SemaphoreType.DMA

    def accumulators(count):
        return [[[pltpu.ACC(b % 2)((rows_b, TILE), jnp.float32) for _ in range(count)]
                 for b in range(batch)] for _ in range(n_head)]

    pl.run_scoped(
        lambda *scoped: kernel(n_seq, n_head, *scoped, *refs),
        accumulators(slots * BLK // TILE), accumulators(width // TILE),
        dma((3,)), dma((n_head * (slots * BLK // TILE + 1),)), dma(()), dma(()), dma(()),
    )


def solution(mesh):
    n_seq, n_head = mesh.shape["seq"], mesh.shape["head"]
    n_all = n_seq * n_head

    def on_device(key_cache, value_cache, query, lengths, block_map):
        batch, slots, _, channels = key_cache.shape
        width = channels // n_head
        rows_b = (width // HD) * REP
        rows = batch * rows_b
        dma = pltpu.SemaphoreType.DMA
        result = pl.pallas_call(
            functools.partial(with_accumulators, n_seq, n_head),
            out_shape=pltpu.VMEM((rows, HD), jnp.bfloat16),
            in_specs=[
                *[pl.BlockSpec(memory_space=pl.ANY)] * 5,
            ],
            out_specs=pl.BlockSpec(memory_space=pltpu.VMEM),
            scratch_shapes=[
                pltpu.SMEM(lengths.shape, jnp.int32),
                pltpu.SMEM(block_map.shape, jnp.int32),
                pltpu.VMEM(query.shape, jnp.bfloat16),
                pltpu.VMEM((n_head, batch, slots, BLK, width), jnp.bfloat16),
                pltpu.VMEM((n_head, batch, slots, BLK, width), jnp.bfloat16),
                pltpu.VMEM(query.shape, jnp.bfloat16),
                pltpu.VMEM((n_head, rows, HD), jnp.bfloat16),
                pltpu.VMEM((n_head, HD), jnp.float32),
                pltpu.VMEM((n_all, rows, HD), jnp.bfloat16),
                pltpu.VMEM((n_all, HD), jnp.float32),
                pltpu.VMEM((n_all, rows, HD), jnp.float32),
                pltpu.VMEM((rows, HD), jnp.float32),
                dma(()),
                dma(()),
                dma(()),
                pltpu.SemaphoreType.REGULAR,
            ],
            compiler_params=pltpu.CompilerParams(collective_id=0, has_side_effects=True),
        )(lengths, block_map, query, key_cache, value_cache)
        return result.reshape(rows_b, batch, HD).transpose(1, 0, 2).reshape(batch, rows_b * HD)

    placed = (
        P("grp", ("seq", "head"), None, None),
        P("grp", ("seq", "head"), None, None),
        P("grp", "head"),
        P("grp"),
        P("grp", None),
    )
    return jax.shard_map(
        on_device, mesh=mesh, in_specs=placed, out_specs=P("grp", "head"), check_vma=False
    )
```

```python
import functools

import jax
import jax.numpy as jnp
from jax import lax
from jax.experimental import pallas as pl
from jax.experimental.pallas import tpu as pltpu
from jax.sharding import PartitionSpec as P

QH = 32
KVH = 8
HD = 128
BLK = 128
TILE = 256
REP = QH // KVH
MESH = pl.DeviceIdType.MESH
NEG = -1e30
LOG2E = 1.4426950408889634


def kernel(
    n_seq, n_head, score_acc, value_acc, small_sem, kv_sem, qsend_sem, nsend_sem, ssend_sem,
    lengths_hbm, map_hbm, q_hbm, k_hbm, v_hbm, out_ref,
    lengths, block_map, q_ref,
    k_buf, v_buf, q_mate, num_send, stat_send, num_recv, stat_recv, share_ref, order_ref,
    q_sem, nrecv_sem, srecv_sem, ready_sem,
):
    seq = lax.axis_index("seq")
    head = lax.axis_index("head")
    batch, slots = k_hbm.shape[0], k_hbm.shape[1]
    width = k_hbm.shape[3] // n_head
    groups = width // HD
    rows_b = groups * REP
    rows = batch * rows_b
    tokens = slots * BLK
    per = TILE // BLK
    pieces = tokens // TILE
    strips = width // TILE
    me = seq * n_head + head
    mate = n_head - 1 - head
    n_all = n_seq * n_head
    small = n_all <= 16

    def loop(lo, hi, body):
        if small:
            for i in range(lo, hi):
                body(i)
        else:
            def step(i, carry):
                body(i)
                return carry
            lax.fori_loop(lo, hi, step, 0)

    def turned(d):
        return jnp.where(d == n_seq - 1, seq, d + jnp.where(d >= seq, 1, 0))

    smalls = [pltpu.make_async_copy(a, b, small_sem.at[i]) for i, (a, b) in enumerate(
        ((lengths_hbm, lengths), (map_hbm, block_map), (q_hbm, q_ref)))]

    def load(half, which, piece=None):
        owner = jnp.where(half == 0, head, mate)
        source, target = ((k_hbm, k_buf), (v_hbm, v_buf))[which]
        lanes = pl.ds(pl.multiple_of(owner * width, width), width)
        blocks = pl.ds(0, slots) if piece is None else pl.ds(piece * per, per)
        return pltpu.make_async_copy(
            source.at[:, blocks, :, lanes], target.at[half, :, blocks],
            kv_sem.at[half * (pieces + 1) + (pieces if piece is None else piece)],
        )

    for copy in smalls:
        copy.start()
    for piece in range(pieces):
        load(0, 0, piece).start()
    load(0, 1).start(priority=1)

    barrier = pltpu.get_barrier_semaphore()
    lead = head == n_head - 1

    def q_copy():
        return pltpu.make_async_remote_copy(
            src_ref=q_ref, dst_ref=q_mate, send_sem=qsend_sem, recv_sem=q_sem,
            device_id={"head": mate}, device_id_type=MESH,
        )

    def tell_mate():
        pl.semaphore_signal(ready_sem, inc=1, device_id={"head": mate}, device_id_type=MESH)

    @pl.when(lead)
    def _():
        pl.semaphore_signal(barrier, inc=1, device_id={"head": mate}, device_id_type=MESH)
        pl.semaphore_wait(ready_sem, 1)

        def greet(d):
            pl.semaphore_signal(barrier, inc=1, device_id={"seq": turned(d)}, device_id_type=MESH)

        loop(0, n_seq - 1, greet)

    @pl.when(jnp.logical_not(lead))
    def _():
        pl.semaphore_wait(barrier, 1)
        tell_mate()

    smalls[2].wait()
    q_copy().start()

    def everyone_in():
        @pl.when(lead)
        def _():
            pl.semaphore_wait(barrier, n_seq - 1)
            tell_mate()

        @pl.when(jnp.logical_not(lead))
        def _():
            pl.semaphore_wait(ready_sem, 1)

    def bias_of(b):
        parts = []
        for j in range(slots):
            here = block_map[b, me * slots + j] * BLK < lengths[b]
            parts.append(jnp.broadcast_to(jnp.where(here, 0.0, NEG), (rows_b, BLK)))
        return jnp.concatenate(parts, axis=1)

    def diagonal(q):
        lifted = q.astype(jnp.float32).reshape(rows, HD)
        wide = jnp.concatenate([lifted] * groups, axis=1)
        row_group = lax.rem(lax.broadcasted_iota(jnp.int32, wide.shape, 0), rows_b) // REP
        lane_group = lax.broadcasted_iota(jnp.int32, wide.shape, 1) // HD
        return jnp.where(row_group == lane_group, wide, 0.0).astype(jnp.bfloat16)

    for copy in smalls[:2]:
        copy.wait()
    for piece in range(pieces):
        load(1, 0, piece).start()
    load(1, 1).start(priority=1)
    bias = [bias_of(b) for b in range(batch)]

    def copies(half, d):
        where = {"seq": turned(d), "head": mate if half else head}
        return (
            pltpu.make_async_remote_copy(
                src_ref=stat_send.at[pl.ds(half, 1)], dst_ref=stat_recv.at[pl.ds(me, 1)],
                send_sem=ssend_sem, recv_sem=srecv_sem, device_id=where, device_id_type=MESH,
            ),
            pltpu.make_async_remote_copy(
                src_ref=num_send.at[half], dst_ref=num_recv.at[me],
                send_sem=nsend_sem, recv_sem=nrecv_sem, device_id=where, device_id_type=MESH,
            ),
        )

    def send(half, which, turns):
        loop(*turns, lambda d: copies(half, d)[which].start())

    row_group = lax.broadcasted_iota(jnp.int32, (rows_b, HD), 0) // REP
    row = lax.broadcasted_iota(jnp.int32, (rows, HD), 0)
    lane = lax.broadcasted_iota(jnp.int32, (rows, HD), 1)

    def push(ref, half, b, i):
        t, c = i // strips, i % strips
        tile = ref[half, b, t * per:(t + 1) * per, :, c * TILE:(c + 1) * TILE].reshape(TILE, TILE)
        pltpu.matmul_push_rhs(tile, i % 2, b % 2, transpose=ref is k_buf)

    def fill(ref, half, lo, hi):
        for i in range(lo, hi):
            for b in range(batch):
                push(ref, half, b, i)

    def score(half, spread, t):
        for i in range(t * strips, (t + 1) * strips):
            for b in range(batch):
                c = i % strips
                lhs = spread[b * rows_b:(b + 1) * rows_b, c * TILE:(c + 1) * TILE]
                pltpu.matmul_acc_lhs(score_acc[half][b][t], lhs, load_staged_rhs=i % 2)

    def peak(half):
        scores = []
        for b in range(batch):
            raw = jnp.concatenate([pltpu.matmul_pop(acc) for acc in score_acc[half][b]], axis=1)
            scores.append(raw * (LOG2E / HD**0.5) + bias[b])
        return [(x, jnp.max(x, axis=1, keepdims=True)) for x in scores]

    def soften(peaks):
        return [(jnp.exp2(x - top), top) for x, top in peaks]

    def note(half, soft):
        totals = [jnp.sum(expo, axis=1, keepdims=True) for expo, _ in soft]
        record = jnp.where(lane == row, jnp.concatenate([top for _, top in soft], axis=0), 0.0)
        record = jnp.where(lane == row + rows, jnp.concatenate(totals, axis=0), record)
        stat_send[half:half + 1] = jnp.sum(record, axis=0, keepdims=True)

    def weigh(half, soft):
        expos = [expo.astype(jnp.bfloat16) for expo, _ in soft]
        for i in range(pieces * strips):
            t, c = i // strips, i % strips
            for b in range(batch):
                pltpu.matmul_acc_lhs(
                    value_acc[half][b][c], expos[b][:, t * TILE:(t + 1) * TILE], load_staged_rhs=i % 2)
            if i + 2 < pieces * strips:
                fill(v_buf, half, i + 2, i + 3)

    def finish(half):
        nums = []
        for b in range(batch):
            part = jnp.zeros((rows_b, HD), jnp.float32)
            for c in range(strips):
                full = pltpu.matmul_pop(value_acc[half][b][c])
                for g in range(TILE // HD):
                    part = jnp.where(row_group == c * (TILE // HD) + g, full[:, g * HD:(g + 1) * HD], part)
            nums.append(part)
        num_send[half] = jnp.concatenate(nums, axis=0).astype(jnp.bfloat16)

    own_turns, mate_turns, first = (0, n_seq - 1), (0, n_seq), max(1, n_seq // 4)
    spread = diagonal(q_ref[...])
    for t in range(pieces):
        load(0, 0, t).wait()
        fill(k_buf, 0, t * strips, (t + 1) * strips)
        score(0, spread, t)
    peaks = peak(0)
    soft = soften(peaks)
    load(0, 1).wait()
    fill(v_buf, 0, 0, 2)
    weigh(0, soft)
    note(0, soft)
    everyone_in()
    send(0, 0, (0, first))
    finish(0)
    send(0, 1, (0, first))
    load(1, 0, 0).wait()
    fill(k_buf, 1, 0, strips)
    q_copy().wait()
    spread = diagonal(q_mate[...])
    score(1, spread, 0)
    for t in range(1, pieces):
        load(1, 0, t).wait()
        fill(k_buf, 1, t * strips, (t + 1) * strips)
        score(1, spread, t)
    peaks = peak(1)
    soft = soften(peaks)
    load(1, 1).wait()
    fill(v_buf, 1, 0, 2)
    weigh(1, soft)
    note(1, soft)
    send(1, 0, (0, first))
    finish(1)
    send(1, 1, (0, first))
    send(0, 0, (first, n_seq - 1))
    send(1, 0, (first, n_seq))
    send(0, 1, (first, n_seq - 1))
    send(1, 1, (first, n_seq))

    all_nums = pltpu.make_async_remote_copy(
        src_ref=num_recv.at[pl.ds(0, n_all - 1)], dst_ref=num_recv.at[pl.ds(0, n_all - 1)],
        send_sem=nsend_sem, recv_sem=nrecv_sem, device_id={"head": mate}, device_id_type=MESH,
    )
    all_stats = pltpu.make_async_remote_copy(
        src_ref=stat_recv.at[pl.ds(0, n_all - 1)], dst_ref=stat_recv.at[pl.ds(0, n_all - 1)],
        send_sem=ssend_sem, recv_sem=srecv_sem, device_id={"head": mate}, device_id_type=MESH,
    )
    all_stats.wait_send()
    all_nums.wait_send()
    stat_recv[pl.ds(me, 1)] = stat_send[0:1]
    num_recv[me] = num_send[0]
    all_stats.wait_recv()
    stats = stat_recv[...]
    factor = jnp.exp2(stats - jnp.max(stats, axis=0, keepdims=True))

    def column(line):
        return jnp.sum(jnp.where(lane == row, line, 0.0), axis=1, keepdims=True)

    for s in range(n_all):
        share_ref[s] = jnp.broadcast_to(column(factor[s:s + 1]), (rows, HD))
    whole = jnp.sum(factor[:, :rows] * stats[:, rows:2 * rows], axis=0, keepdims=True)
    whole = jnp.concatenate([whole, jnp.ones((1, HD - rows), jnp.float32)], axis=1)
    scale = column(1.0 / whole)
    all_nums.wait_recv()

    def term(s):
        return share_ref[s] * num_recv[s].astype(jnp.float32)

    if small:
        terms = [term(s) for s in range(n_all)]
        while len(terms) > 1:
            terms = [a + b for a, b in zip(terms[::2], terms[1::2])] + terms[len(terms) // 2 * 2:]
        result = terms[0]
    else:
        result = lax.fori_loop(0, n_all, lambda s, acc: acc + term(s), jnp.zeros((rows, HD), jnp.float32))
    result = result * scale
    for b in range(batch):
        order_ref[pl.ds(b, rows_b, stride=batch), :] = result[b * rows_b:(b + 1) * rows_b]
    out_ref[...] = order_ref[...].astype(out_ref.dtype)


def with_accumulators(n_seq, n_head, *refs):
    batch, slots = refs[3].shape[0], refs[3].shape[1]
    width = refs[3].shape[3] // n_head
    rows_b = width // HD * REP
    dma = pltpu.SemaphoreType.DMA

    def accumulators(count):
        return [[[pltpu.ACC(b % 2)((rows_b, TILE), jnp.float32) for _ in range(count)]
                 for b in range(batch)] for _ in range(n_head)]

    pl.run_scoped(
        lambda *scoped: kernel(n_seq, n_head, *scoped, *refs),
        accumulators(slots * BLK // TILE), accumulators(width // TILE),
        dma((3,)), dma((n_head * (slots * BLK // TILE + 1),)), dma(()), dma(()), dma(()),
    )


def solution(mesh):
    n_seq, n_head = mesh.shape["seq"], mesh.shape["head"]
    n_all = n_seq * n_head

    def on_device(key_cache, value_cache, query, lengths, block_map):
        batch, slots, _, channels = key_cache.shape
        width = channels // n_head
        rows_b = (width // HD) * REP
        rows = batch * rows_b
        dma = pltpu.SemaphoreType.DMA
        result = pl.pallas_call(
            functools.partial(with_accumulators, n_seq, n_head),
            out_shape=pltpu.VMEM((rows, HD), jnp.bfloat16),
            in_specs=[
                *[pl.BlockSpec(memory_space=pl.ANY)] * 5,
            ],
            out_specs=pl.BlockSpec(memory_space=pltpu.VMEM),
            scratch_shapes=[
                pltpu.SMEM(lengths.shape, jnp.int32),
                pltpu.SMEM(block_map.shape, jnp.int32),
                pltpu.VMEM(query.shape, jnp.bfloat16),
                pltpu.VMEM((n_head, batch, slots, BLK, width), jnp.bfloat16),
                pltpu.VMEM((n_head, batch, slots, BLK, width), jnp.bfloat16),
                pltpu.VMEM(query.shape, jnp.bfloat16),
                pltpu.VMEM((n_head, rows, HD), jnp.bfloat16),
                pltpu.VMEM((n_head, HD), jnp.float32),
                pltpu.VMEM((n_all, rows, HD), jnp.bfloat16),
                pltpu.VMEM((n_all, HD), jnp.float32),
                pltpu.VMEM((n_all, rows, HD), jnp.float32),
                pltpu.VMEM((rows, HD), jnp.float32),
                dma(()),
                dma(()),
                dma(()),
                pltpu.SemaphoreType.REGULAR,
            ],
            compiler_params=pltpu.CompilerParams(collective_id=0, has_side_effects=True),
        )(lengths, block_map, query, key_cache, value_cache)
        return result.reshape(rows_b, batch, HD).transpose(1, 0, 2).reshape(batch, rows_b * HD)

    placed = (
        P("grp", ("seq", "head"), None, None),
        P("grp", ("seq", "head"), None, None),
        P("grp", "head"),
        P("grp"),
        P("grp", None),
    )
    return jax.shard_map(
        on_device, mesh=mesh, in_specs=placed, out_specs=P("grp", "head"), check_vma=False
    )
```

```python
import functools

import jax
import jax.numpy as jnp
from jax import lax
from jax.experimental import pallas as pl
from jax.experimental.pallas import tpu as pltpu
from jax.sharding import PartitionSpec as P

QH = 32
KVH = 8
HD = 128
BLK = 128
TILE = 256
REP = QH // KVH
MESH = pl.DeviceIdType.MESH
NEG = -1e30
LOG2E = 1.4426950408889634


def kernel(
    n_seq, n_head, score_acc, value_acc, small_sem, kv_sem, qsend_sem, nsend_sem, ssend_sem,
    lengths_hbm, map_hbm, q_hbm, k_hbm, v_hbm, out_ref,
    lengths, block_map, q_ref,
    k_buf, v_buf, q_mate, num_send, stat_send, num_recv, stat_recv, share_ref, order_ref,
    q_sem, nrecv_sem, srecv_sem, ready_sem,
):
    seq = lax.axis_index("seq")
    head = lax.axis_index("head")
    batch, slots = k_hbm.shape[0], k_hbm.shape[1]
    width = k_hbm.shape[3] // n_head
    groups = width // HD
    rows_b = groups * REP
    rows = batch * rows_b
    tokens = slots * BLK
    per = TILE // BLK
    pieces = tokens // TILE
    strips = width // TILE
    me = seq * n_head + head
    mate = n_head - 1 - head
    n_all = n_seq * n_head
    small = n_all <= 16

    def loop(lo, hi, body):
        if small:
            for i in range(lo, hi):
                body(i)
        else:
            def step(i, carry):
                body(i)
                return carry
            lax.fori_loop(lo, hi, step, 0)

    def turned(d):
        return jnp.where(d == n_seq - 1, seq, d + jnp.where(d >= seq, 1, 0))

    smalls = [pltpu.make_async_copy(a, b, small_sem.at[i]) for i, (a, b) in enumerate(
        ((lengths_hbm, lengths), (map_hbm, block_map), (q_hbm, q_ref)))]

    def load(half, which, piece=None):
        owner = jnp.where(half == 0, head, mate)
        source, target = ((k_hbm, k_buf), (v_hbm, v_buf))[which]
        lanes = pl.ds(pl.multiple_of(owner * width, width), width)
        blocks = pl.ds(0, slots) if piece is None else pl.ds(piece * per, per)
        return pltpu.make_async_copy(
            source.at[:, blocks, :, lanes], target.at[half, :, blocks],
            kv_sem.at[half * (pieces + 1) + (pieces if piece is None else piece)],
        )

    for copy in smalls:
        copy.start()
    for piece in range(pieces):
        load(0, 0, piece).start()
    load(0, 1).start(priority=0)
    for piece in range(pieces):
        load(1, 0, piece).start(priority=1)

    barrier = pltpu.get_barrier_semaphore()
    lead = head == n_head - 1

    def q_copy():
        return pltpu.make_async_remote_copy(
            src_ref=q_ref, dst_ref=q_mate, send_sem=qsend_sem, recv_sem=q_sem,
            device_id={"head": mate}, device_id_type=MESH,
        )

    def tell_mate():
        pl.semaphore_signal(ready_sem, inc=1, device_id={"head": mate}, device_id_type=MESH)

    @pl.when(lead)
    def _():
        pl.semaphore_signal(barrier, inc=1, device_id={"head": mate}, device_id_type=MESH)
        pl.semaphore_wait(ready_sem, 1)

        def greet(d):
            pl.semaphore_signal(barrier, inc=1, device_id={"seq": turned(d)}, device_id_type=MESH)

        loop(0, n_seq - 1, greet)

    @pl.when(jnp.logical_not(lead))
    def _():
        pl.semaphore_wait(barrier, 1)
        tell_mate()

    smalls[2].wait()
    q_copy().start()

    def everyone_in():
        @pl.when(lead)
        def _():
            pl.semaphore_wait(barrier, n_seq - 1)
            tell_mate()

        @pl.when(jnp.logical_not(lead))
        def _():
            pl.semaphore_wait(ready_sem, 1)

    def bias_of(b):
        parts = []
        for j in range(slots):
            here = block_map[b, me * slots + j] * BLK < lengths[b]
            parts.append(jnp.broadcast_to(jnp.where(here, 0.0, NEG), (rows_b, BLK)))
        return jnp.concatenate(parts, axis=1)

    def diagonal(q):
        lifted = q.astype(jnp.float32).reshape(rows, HD)
        wide = jnp.concatenate([lifted] * groups, axis=1)
        row_group = lax.rem(lax.broadcasted_iota(jnp.int32, wide.shape, 0), rows_b) // REP
        lane_group = lax.broadcasted_iota(jnp.int32, wide.shape, 1) // HD
        return jnp.where(row_group == lane_group, wide, 0.0).astype(jnp.bfloat16)

    for copy in smalls[:2]:
        copy.wait()
    load(1, 1).start(priority=1)
    bias = [bias_of(b) for b in range(batch)]

    def copies(half, d):
        where = {"seq": turned(d), "head": mate if half else head}
        return (
            pltpu.make_async_remote_copy(
                src_ref=stat_send.at[pl.ds(half, 1)], dst_ref=stat_recv.at[pl.ds(me, 1)],
                send_sem=ssend_sem, recv_sem=srecv_sem, device_id=where, device_id_type=MESH,
            ),
            pltpu.make_async_remote_copy(
                src_ref=num_send.at[half], dst_ref=num_recv.at[me],
                send_sem=nsend_sem, recv_sem=nrecv_sem, device_id=where, device_id_type=MESH,
            ),
        )

    def send(half, which, turns):
        loop(*turns, lambda d: copies(half, d)[which].start())

    row_group = lax.broadcasted_iota(jnp.int32, (rows_b, HD), 0) // REP
    row = lax.broadcasted_iota(jnp.int32, (rows, HD), 0)
    lane = lax.broadcasted_iota(jnp.int32, (rows, HD), 1)

    def multiply(acc, b, lhs, rhs, transpose):
        register = turn[b % 2]
        turn[b % 2] = 1 - register
        pltpu.matmul_push_rhs(rhs, register, b % 2, transpose=transpose)
        pltpu.matmul_acc_lhs(acc, lhs, load_staged_rhs=register)

    turn = [0, 0]

    def score(half, spread, t):
        for c in range(strips):
            for b in range(batch):
                keys = k_buf[half, b, t * per:(t + 1) * per, :, c * TILE:(c + 1) * TILE]
                multiply(
                    score_acc[half][b][t], b, spread[b * rows_b:(b + 1) * rows_b, c * TILE:(c + 1) * TILE],
                    keys.reshape(TILE, TILE), True,
                )

    def soften(half):
        soft = []
        for b in range(batch):
            raw = jnp.concatenate([pltpu.matmul_pop(acc) for acc in score_acc[half][b]], axis=1)
            scores = raw * (LOG2E / HD**0.5) + bias[b]
            top = jnp.max(scores, axis=1, keepdims=True)
            soft.append((jnp.exp2(scores - top), top))
        return soft

    def note(half, soft):
        totals = [jnp.sum(expo, axis=1, keepdims=True) for expo, _ in soft]
        record = jnp.where(lane == row, jnp.concatenate([top for _, top in soft], axis=0), 0.0)
        record = jnp.where(lane == row + rows, jnp.concatenate(totals, axis=0), record)
        stat_send[half:half + 1] = jnp.sum(record, axis=0, keepdims=True)

    def weigh(half, soft):
        expos = [expo.astype(jnp.bfloat16) for expo, _ in soft]
        for t in range(pieces):
            for c in range(strips):
                for b in range(batch):
                    values = v_buf[half, b, t * per:(t + 1) * per, :, c * TILE:(c + 1) * TILE]
                    multiply(
                        value_acc[half][b][c], b, expos[b][:, t * TILE:(t + 1) * TILE],
                        values.reshape(TILE, TILE), False,
                    )

    def finish(half):
        nums = []
        for b in range(batch):
            part = jnp.zeros((rows_b, HD), jnp.float32)
            for c in range(strips):
                full = pltpu.matmul_pop(value_acc[half][b][c])
                for g in range(TILE // HD):
                    part = jnp.where(row_group == c * (TILE // HD) + g, full[:, g * HD:(g + 1) * HD], part)
            nums.append(part)
        num_send[half] = jnp.concatenate(nums, axis=0).astype(jnp.bfloat16)

    own_turns, mate_turns, first = (0, n_seq - 1), (0, n_seq), max(1, n_seq // 4)
    spread = diagonal(q_ref[...])
    for t in range(pieces):
        load(0, 0, t).wait()
        score(0, spread, t)
    soft = soften(0)
    load(0, 1).wait()
    weigh(0, soft)
    note(0, soft)
    everyone_in()
    send(0, 0, (0, first))
    q_copy().wait()
    spread = diagonal(q_mate[...])
    load(1, 0, 0).wait()
    score(1, spread, 0)
    finish(0)
    send(0, 1, (0, first))
    for t in range(1, pieces):
        load(1, 0, t).wait()
        score(1, spread, t)
    soft = soften(1)
    load(1, 1).wait()
    weigh(1, soft)
    note(1, soft)
    send(1, 0, (0, first))
    finish(1)
    send(1, 1, (0, first))
    send(0, 0, (first, n_seq - 1))
    send(1, 0, (first, n_seq))
    send(0, 1, (first, n_seq - 1))
    send(1, 1, (first, n_seq))

    all_nums = pltpu.make_async_remote_copy(
        src_ref=num_recv.at[pl.ds(0, n_all - 1)], dst_ref=num_recv.at[pl.ds(0, n_all - 1)],
        send_sem=nsend_sem, recv_sem=nrecv_sem, device_id={"head": mate}, device_id_type=MESH,
    )
    all_stats = pltpu.make_async_remote_copy(
        src_ref=stat_recv.at[pl.ds(0, n_all - 1)], dst_ref=stat_recv.at[pl.ds(0, n_all - 1)],
        send_sem=ssend_sem, recv_sem=srecv_sem, device_id={"head": mate}, device_id_type=MESH,
    )
    all_stats.wait_send()
    all_nums.wait_send()
    stat_recv[pl.ds(me, 1)] = stat_send[0:1]
    num_recv[me] = num_send[0]
    all_stats.wait_recv()
    stats = stat_recv[...]
    factor = jnp.exp2(stats - jnp.max(stats, axis=0, keepdims=True))

    def column(line):
        return jnp.sum(jnp.where(lane == row, line, 0.0), axis=1, keepdims=True)

    for s in range(n_all):
        share_ref[s] = jnp.broadcast_to(column(factor[s:s + 1]), (rows, HD))
    whole = jnp.sum(factor[:, :rows] * stats[:, rows:2 * rows], axis=0, keepdims=True)
    whole = jnp.concatenate([whole, jnp.ones((1, HD - rows), jnp.float32)], axis=1)
    scale = column(1.0 / whole)
    all_nums.wait_recv()

    def term(s):
        return share_ref[s] * num_recv[s].astype(jnp.float32)

    if small:
        terms = [term(s) for s in range(n_all)]
        while len(terms) > 1:
            terms = [a + b for a, b in zip(terms[::2], terms[1::2])] + terms[len(terms) // 2 * 2:]
        result = terms[0]
    else:
        result = lax.fori_loop(0, n_all, lambda s, acc: acc + term(s), jnp.zeros((rows, HD), jnp.float32))
    result = result * scale
    for b in range(batch):
        order_ref[pl.ds(b, rows_b, stride=batch), :] = result[b * rows_b:(b + 1) * rows_b]
    out_ref[...] = order_ref[...].astype(out_ref.dtype)


def with_accumulators(n_seq, n_head, *refs):
    batch, slots = refs[3].shape[0], refs[3].shape[1]
    width = refs[3].shape[3] // n_head
    rows_b = width // HD * REP
    dma = pltpu.SemaphoreType.DMA

    def accumulators(count):
        return [[[pltpu.ACC(b % 2)((rows_b, TILE), jnp.float32) for _ in range(count)]
                 for b in range(batch)] for _ in range(n_head)]

    pl.run_scoped(
        lambda *scoped: kernel(n_seq, n_head, *scoped, *refs),
        accumulators(slots * BLK // TILE), accumulators(width // TILE),
        dma((3,)), dma((n_head * (slots * BLK // TILE + 1),)), dma(()), dma(()), dma(()),
    )


def solution(mesh):
    n_seq, n_head = mesh.shape["seq"], mesh.shape["head"]
    n_all = n_seq * n_head

    def on_device(key_cache, value_cache, query, lengths, block_map):
        batch, slots, _, channels = key_cache.shape
        width = channels // n_head
        rows_b = (width // HD) * REP
        rows = batch * rows_b
        dma = pltpu.SemaphoreType.DMA
        result = pl.pallas_call(
            functools.partial(with_accumulators, n_seq, n_head),
            out_shape=pltpu.VMEM((rows, HD), jnp.bfloat16),
            in_specs=[
                *[pl.BlockSpec(memory_space=pl.ANY)] * 5,
            ],
            out_specs=pl.BlockSpec(memory_space=pltpu.VMEM),
            scratch_shapes=[
                pltpu.SMEM(lengths.shape, jnp.int32),
                pltpu.SMEM(block_map.shape, jnp.int32),
                pltpu.VMEM(query.shape, jnp.bfloat16),
                pltpu.VMEM((n_head, batch, slots, BLK, width), jnp.bfloat16),
                pltpu.VMEM((n_head, batch, slots, BLK, width), jnp.bfloat16),
                pltpu.VMEM(query.shape, jnp.bfloat16),
                pltpu.VMEM((n_head, rows, HD), jnp.bfloat16),
                pltpu.VMEM((n_head, HD), jnp.float32),
                pltpu.VMEM((n_all, rows, HD), jnp.bfloat16),
                pltpu.VMEM((n_all, HD), jnp.float32),
                pltpu.VMEM((n_all, rows, HD), jnp.float32),
                pltpu.VMEM((rows, HD), jnp.float32),
                dma(()),
                dma(()),
                dma(()),
                pltpu.SemaphoreType.REGULAR,
            ],
            compiler_params=pltpu.CompilerParams(collective_id=0, has_side_effects=True),
        )(lengths, block_map, query, key_cache, value_cache)
        return result.reshape(rows_b, batch, HD).transpose(1, 0, 2).reshape(batch, rows_b * HD)

    placed = (
        P("grp", ("seq", "head"), None, None),
        P("grp", ("seq", "head"), None, None),
        P("grp", "head"),
        P("grp"),
        P("grp", None),
    )
    return jax.shard_map(
        on_device, mesh=mesh, in_specs=placed, out_specs=P("grp", "head"), check_vma=False
    )
```
